32 devices in a mesh: batch: 1 (over z), col: 4 (over y), row: 8 (over x, core).
Axes of the slice: x: 4, y: 4, z: 1, core: 2. Of those that a mesh axis runs over, the one named last changes fastest.
The devices are a block of a 4x4x8 slice.
Arguments:
- x: bfloat16 [16, 768, 32, 128], P('batch', 'row', 'col')
- w_down_1: bfloat16 [3, 3, 128, 256], replicated
- b_down_1: float32 [256], replicated
- w_conv_1: bfloat16 [3, 3, 256, 256], replicated
- b_conv_1: float32 [256], replicated
- w_proj_1: bfloat16 [128, 256], replicated
- w_down_2: bfloat16 [3, 3, 256, 320], replicated
- b_down_2: float32 [320], replicated
- w_conv_2: bfloat16 [3, 3, 320, 320], replicated
- b_conv_2: float32 [320], replicated
- w_proj_2: bfloat16 [256, 320], replicated
- w_down_3: bfloat16 [3, 3, 320, 320], replicated
- b_down_3: float32 [320], replicated
- w_conv_3: bfloat16 [3, 3, 320, 320], replicated
- b_conv_3: float32 [320], replicated
- w_proj_3: bfloat16 [320, 320], replicated
Outputs:
- output: bfloat16 [16, 96, 4, 320], P('batch', 'row', 'col')
All inputs are finite; a program needn't handle non-finite values.
Results may differ from the reference program's by a relative error of at most 0.00483591.
Values are sent between devices in bfloat16 or wider.
A program may use at most 768 MiB of HBM per device.

```python
import jax
import jax.numpy as jnp
from jax import lax

IMAGES = 16
TILE_H = 96
TILE_W = 8
ROW_DEVS = 8
COL_DEVS = 4
CHAN_0 = 128
CHAN_1 = 256
CHAN_2 = 320
CHAN_3 = 320
HEIGHT = TILE_H * ROW_DEVS
WIDTH = TILE_W * COL_DEVS
CONV_DIMS = ("NHWC", "HWIO", "NHWC")


def setup_inputs(seed: int = 0, part: int = 0) -> dict:
    root_key = jax.random.key(seed)
    image_key = jax.random.fold_in(jax.random.fold_in(root_key, 1), part)
    inputs = {"x": jax.random.normal(image_key, (IMAGES, HEIGHT, WIDTH, CHAN_0), jnp.float32).astype(jnp.bfloat16)}
    widths = (CHAN_0, CHAN_1, CHAN_2, CHAN_3)
    for stage in range(3):
        c_in = widths[stage]
        c_out = widths[stage + 1]
        stage_keys = jax.random.split(jax.random.fold_in(root_key, 10 + stage), 5)
        suffix = str(stage + 1)
        inputs["w_down_" + suffix] = (jax.random.normal(stage_keys[0], (3, 3, c_in, c_out), jnp.float32) * (9 * c_in) ** -0.5).astype(jnp.bfloat16)
        inputs["b_down_" + suffix] = 0.5 * jax.random.normal(stage_keys[1], (c_out,), jnp.float32)
        inputs["w_conv_" + suffix] = (jax.random.normal(stage_keys[2], (3, 3, c_out, c_out), jnp.float32) * (9 * c_out) ** -0.5).astype(jnp.bfloat16)
        inputs["b_conv_" + suffix] = 0.5 * jax.random.normal(stage_keys[3], (c_out,), jnp.float32)
        inputs["w_proj_" + suffix] = (jax.random.normal(stage_keys[4], (c_in, c_out), jnp.float32) * c_in ** -0.5).astype(jnp.bfloat16)
    return inputs


def conv_same(act_in, weight, stride):
    return lax.conv_general_dilated(act_in.astype(jnp.float32), weight.astype(jnp.float32), (stride, stride), ((1, 1), (1, 1)), dimension_numbers=CONV_DIMS)


def basic_block(z_prev, w_down, b_down, w_conv, b_conv, w_proj):
    y_act = jax.nn.relu(conv_same(z_prev, w_down, 2) + b_down).astype(jnp.bfloat16)
    shortcut = jnp.einsum("bhwc,cd->bhwd", z_prev[:, ::2, ::2].astype(jnp.float32), w_proj.astype(jnp.float32))
    return jax.nn.relu(conv_same(y_act, w_conv, 1) + shortcut + b_conv).astype(jnp.bfloat16)


def reference(x, w_down_1, b_down_1, w_conv_1, b_conv_1, w_proj_1, w_down_2, b_down_2, w_conv_2, b_conv_2, w_proj_2, w_down_3, b_down_3, w_conv_3, b_conv_3, w_proj_3):
    params = ((w_down_1, b_down_1, w_conv_1, b_conv_1, w_proj_1), (w_down_2, b_down_2, w_conv_2, b_conv_2, w_proj_2), (w_down_3, b_down_3, w_conv_3, b_conv_3, w_proj_3))

    def one_image(image):
        act_out = image[None]
        for stage_params in params:
            act_out = basic_block(act_out, stage_params[0], stage_params[1], stage_params[2], stage_params[3], stage_params[4])
        return act_out[0]

    return lax.map(one_image, x)
```

```python
import functools

import jax
import jax.numpy as jnp
from jax import lax
from jax.experimental import pallas as pl
from jax.experimental.pallas import tpu as pltpu
from jax.sharding import PartitionSpec as P

LANE = 128
MESH = pl.DeviceIdType.MESH
NEIGHBOURS = [(dr, dc) for dr in (-1, 0, 1) for dc in (-1, 0, 1) if (dr, dc) != (0, 0)]


def tiles_of(channels):
    return -(-channels // LANE)


def cut(count, pieces, unit=1):
    bounds = [round(count * k / pieces / unit) * unit for k in range(pieces + 1)]
    return [(a, b) for a, b in zip(bounds, bounds[1:]) if b > a]


class Exchange:
    def __init__(self, grid, sems, counter):
        self.grid, self.sems, self.counter = grid, sems, counter
        self.copies = {}
        self.waited = set()

    def exists(self, dr, dc):
        row, col, row_count, col_count = self.grid
        tests = []
        if dr == 1:
            tests.append(row + 1 < row_count)
        if dr == -1:
            tests.append(row > 0)
        if dc == 1:
            tests.append(col + 1 < col_count)
        if dc == -1:
            tests.append(col > 0)
        return functools.reduce(jnp.logical_and, tests)

    def send(self, key, dr, dc, src, dst):
        row, col = self.grid[:2]
        index = self.counter[0]
        self.counter[0] += 1
        copy = pltpu.make_async_remote_copy(
            src_ref=src, dst_ref=dst, send_sem=self.sems.at[0, index], recv_sem=self.sems.at[1, index],
            device_id={"row": row + dr, "col": col + dc}, device_id_type=MESH)
        self.copies[key] = (copy, dr, dc)
        pl.when(self.exists(dr, dc))(copy.start)

    def need(self, *keys):
        for key in keys:
            if key not in self.waited:
                self.waited.add(key)
                copy, dr, dc = self.copies[key]
                pl.when(self.exists(-dr, -dc))(copy.wait_recv)

    def finish(self):
        assert self.waited == set(self.copies)
        for copy, dr, dc in self.copies.values():
            pl.when(self.exists(dr, dc))(copy.wait_send)


def body(cfg, x_hbm, *refs):
    params, refs = refs[:15], refs[15:]
    out_ref, xs, ys, zs, ws, load_sems, sems = refs[0], refs[1], refs[2:5], refs[5:7], refs[7:16], refs[16], refs[17]
    chans, height, width = cfg["chans"], cfg["height"], cfg["width"]
    row, col = lax.axis_index("row"), lax.axis_index("col")
    grid = (row, col, cfg["rows"], cfg["cols"])
    counter = [0]
    dtype = jnp.bfloat16
    images = cfg["images"]

    loads = [pltpu.make_async_copy(x_hbm, xs.at[0, 1:, :, 1:], load_sems.at[0])]
    for stage in range(3):
        for k, p in enumerate((0, 2, 4)):
            src, dst = params[5 * stage + p], ws[3 * stage + k]
            if dst.shape != src.shape:
                dst = dst.at[:, :src.shape[1]]
            loads.append(pltpu.make_async_copy(src, dst, load_sems.at[1 + 3 * stage + k]))
    for load in loads[:4]:
        load.start()

    def zero(ref):
        ref[...] = jnp.zeros(ref.shape, ref.dtype)

    for buf in (xs,) + tuple(zs):
        zero(buf.at[:, 0, 1])
        zero(buf.at[:, :, :, 0, 1])
    for buf in ys:
        zero(buf.at[:, 0:1])
        zero(buf.at[:, -1:])
        zero(buf.at[:, :, 0:1])
        zero(buf.at[:, :, -1:])
    for buf in tuple(ys[1:]) + tuple(zs[1:]):
        zero(buf.at[buf.shape[0] - 1:])
    for k, p in enumerate((0, 2, 4) * 3):
        src, dst = params[5 * (k // 3) + p], ws[k]
        if dst.shape != src.shape:
            zero(dst.at[:, src.shape[1]:])

    for load in loads[4:]:
        load.start()

    exchanges = [Exchange(grid, sems, counter) for _ in range(6)]
    barrier = pltpu.get_barrier_semaphore()
    for dr, dc in NEIGHBOURS:
        there = exchanges[0].exists(dr, dc)

        def greet(dr=dr, dc=dc):
            pl.semaphore_signal(barrier, inc=1, device_id={"row": row + dr, "col": col + dc}, device_id_type=MESH)

        pl.when(there)(greet)
    row_inner = jnp.logical_and(row > 0, row + 1 < cfg["rows"])
    col_inner = jnp.logical_and(col > 0, col + 1 < cfg["cols"])
    for row_peers, row_test in ((3, row_inner), (2, jnp.logical_not(row_inner))):
        for col_peers, col_test in ((3, col_inner), (2, jnp.logical_not(col_inner))):
            peers = row_peers * col_peers - 1
            pl.when(jnp.logical_and(row_test, col_test))(functools.partial(pl.semaphore_wait, barrier, peers))

    zin = [xs, zs[0], zs[1]]

    waited_loads = set()

    def wait_load(index):
        if index not in waited_loads:
            waited_loads.add(index)
            loads[index].wait()

    def flat(block):
        return block.reshape(-1, LANE)

    def stack(pieces):
        return pieces[0] if len(pieces) == 1 else jnp.concatenate(pieces, axis=0)

    def matrix(ref):
        value = ref[...]
        return value.reshape(-1, value.shape[-1])

    def times(lhs, ref, transposed):
        if transposed:
            return sum(lax.dot_general(lhs[:, t * ref.shape[2]:(t + 1) * ref.shape[2]], ref[t], (((1,), (1,)), ((), ())), preferred_element_type=jnp.float32)
                       for t in range(ref.shape[0]))
        return jnp.dot(lhs, matrix(ref), preferred_element_type=jnp.float32)

    def strided(src, ct, runs, kh, kw, c0, c1):
        up, lo = (1 if kh else 0), c0 + (1 if kw else 0)
        return stack([flat(src[ct, a + up:b + up, (kh + 1) % 2, lo:lo + c1 - c0, (kw + 1) % 2]) for a, b in runs])

    def centre(s, runs, c0, c1):
        src = zin[s]
        return jnp.concatenate([strided(src, ct, runs, 1, 1, c0, c1) for ct in range(src.shape[0])], axis=1)

    def down(s, rows, c0, c1):
        src, dst = zin[s], ys[s]
        wait_load(1 + 3 * s)
        taps = []
        for kh in range(3):
            for kw in range(3):
                for ct in range(src.shape[0]):
                    taps.append(strided(src, ct, rows, kh, kw, c0, c1))
        acc = times(jnp.concatenate(taps, axis=1), ws[3 * s], cfg["transposed"][3 * s])
        val = jnp.maximum(acc + params[5 * s + 1][...], 0.0).astype(dtype)
        n = images * (c1 - c0)
        for ct in range(dst.shape[0]):
            l1 = min(chans[s + 1] - ct * LANE, LANE)
            r = 0
            for a, b in rows:
                part = val[r * n:(r + b - a) * n, ct * LANE:ct * LANE + l1]
                dst[ct, a + 1:b + 1, c0 + 1:c1 + 1, :, 0:l1] = part.reshape(b - a, c1 - c0, images, l1)
                r += b - a

    def conv(s, rows, c0, c1):
        src = ys[s]
        wait_load(2 + 3 * s)
        wait_load(3 + 3 * s)
        taps = []
        for kh in range(3):
            for kw in range(3):
                for ct in range(src.shape[0]):
                    taps.append(stack([flat(src[ct, a + kh:b + kh, c0 + kw:c1 + kw]) for a, b in rows]))
        acc = times(jnp.concatenate(taps, axis=1), ws[3 * s + 1], cfg["transposed"][3 * s + 1])
        acc += times(centre(s, rows, c0, c1), ws[3 * s + 2], cfg["transposed"][3 * s + 2])
        val = jnp.maximum(acc + params[5 * s + 3][...], 0.0).astype(dtype)
        n = images * (c1 - c0)
        if s == 2:
            (a, b), = rows
            out_ref[a:b] = val.reshape(b - a, images, chans[3])
            return
        dst = zin[s + 1]
        for ct in range(dst.shape[0]):
            l1 = min(chans[s + 1] - ct * LANE, LANE)
            r = 0
            for a, b in rows:
                part = val[r * n:(r + b - a) * n, ct * LANE:ct * LANE + l1].reshape(b - a, c1 - c0, images, l1)
                r += b - a
                even, odd = a + a % 2, b - b % 2
                for c in range(c0, c1):
                    into = (c // 2 + 1, c % 2, slice(None), slice(0, l1))
                    if a < even:
                        dst[(ct, a // 2 + 1, 1) + into] = part[0, c - c0]
                    if odd > even:
                        dst[(ct, slice(even // 2 + 1, odd // 2 + 1), slice(None)) + into] = part[even - a:odd - a, c - c0].reshape((odd - even) // 2, 2, images, l1)
                    if odd < b and b - 1 >= even:
                        dst[(ct, odd // 2 + 1, 0) + into] = part[b - 1 - a, c - c0]

    def send_y_col(s, side, k, a, b):
        y, w = ys[s], width[s + 1]
        own, there = (w, 0) if side > 0 else (1, w + 1)
        exchanges[2 * s + 1].send(("c", side, k), 0, side, y.at[:, 1 + a:1 + b, own], y.at[:, 1 + a:1 + b, there])

    def send_y_row(s, side):
        y, h, w = ys[s], height[s + 1], width[s + 1]
        own, there = (h, 0) if side > 0 else (1, h + 1)
        ex = exchanges[2 * s + 1]
        ex.send(("r", side), side, 0, y.at[:, own, 1:w + 1], y.at[:, there, 1:w + 1])
        ex.send(("d", side, 1), side, 1, y.at[:, own, w], y.at[:, there, 0])
        ex.send(("d", side, -1), side, -1, y.at[:, own, 1], y.at[:, there, w + 1])

    def send_z_col(s, k, a, b):
        z, w = zin[s], width[s]
        exchanges[2 * s].send(("c", k), 0, 1, z.at[:, 1 + a // 2:1 + b // 2, :, w // 2, 1], z.at[:, 1 + a // 2:1 + b // 2, :, 0, 1])

    def send_z_row(s):
        z, h, w = zin[s], height[s], width[s]
        ex = exchanges[2 * s]
        ex.send("r", 1, 0, z.at[:, h // 2, 1, 1:], z.at[:, 0, 1, 1:])
        ex.send("d", 1, 1, z.at[:, h // 2, 1, w // 2, 1], z.at[:, 0, 1, 0, 1])

    def need_z_col(s, b):
        for k, (lo, hi) in enumerate(zcuts[s]):
            if lo < 2 * b:
                exchanges[2 * s].need(("c", k))

    def need_y_col(s, side, b):
        for k, (lo, hi) in enumerate(ycuts[s]):
            if lo < b + 1:
                exchanges[2 * s + 1].need(("c", side, k))

    def blocks(lo, hi, size):
        return [[(k, min(k + size, hi))] for k in range(lo, hi, size)]

    zcuts = [cut(height[s], cfg["zcut"][s], 2) for s in range(3)]
    ycuts = [cut(height[s + 1], cfg["ycut"][s]) for s in range(3)]

    h0, w0 = height[0], width[0]
    ex = exchanges[0]
    ex.send("r", 1, 0, x_hbm.at[h0 // 2 - 1, 1], xs.at[0, 0, 1, 1:])
    ex.send("d", 1, 1, x_hbm.at[h0 // 2 - 1, 1, w0 // 2 - 1, 1], xs.at[0, 0, 1, 0, 1])
    for k, (a, b) in enumerate(zcuts[0]):
        ex.send(("c", k), 0, 1, x_hbm.at[a // 2:b // 2, :, w0 // 2 - 1, 1], xs.at[0, 1 + a // 2:1 + b // 2, :, 0, 1])
    wait_load(0)

    h1, w1 = height[1], width[1]
    for rows in blocks(8, h1, 8):
        down(0, rows, 1, w1)
    ex.need("r")
    down(0, [(0, 8)], 1, w1)
    for k, (a, b) in enumerate(ycuts[0]):
        send_y_col(0, 1, k, a, b)
    for k, (a, b) in enumerate(ycuts[0]):
        need_z_col(0, b)
        if k == 0:
            ex.need("d")
        down(0, [(a, b)], 0, 1)
        send_y_col(0, -1, k, a, b)
        if k == 0:
            send_y_row(0, -1)
        if b == h1:
            send_y_row(0, 1)
        lo, hi = max(a - 1, 1), b - 1
        for rows in blocks(lo, hi, 8):
            conv(0, rows, 1, w1 - 1)
    ex = exchanges[1]
    ex.need(("r", -1), ("r", 1))
    conv(0, [(0, 1), (h1 - 1, h1)], 1, w1 - 1)
    for k, (a, b) in enumerate(zcuts[1]):
        need_y_col(0, -1, b)
        if k == 0:
            ex.need(("d", 1, -1))
        if b == h1:
            ex.need(("d", -1, -1))
        conv(0, [(a, b)], w1 - 1, w1)
        send_z_col(1, k, a, b)
    for k, (a, b) in enumerate(zcuts[1]):
        need_y_col(0, 1, b)
        if k == 0:
            ex.need(("d", 1, 1))
        if b == h1:
            ex.need(("d", -1, 1))
        conv(0, [(a, b)], 0, 1)
    send_z_row(1)

    for s in (1, 2):
        h, w = height[s + 1], width[s + 1]
        ex = exchanges[2 * s]
        ex.need("r")
        if w > 1:
            for rows in blocks(0, h, 12):
                down(s, rows, 1, w)
            for k, (a, b) in enumerate(ycuts[s]):
                send_y_col(s, 1, k, a, b)
        for k, (a, b) in enumerate(ycuts[s]):
            need_z_col(s, b)
            if k == 0:
                ex.need("d")
            down(s, [(a, b)], 0, 1)
            if w == 1:
                send_y_col(s, 1, k, a, b)
            send_y_col(s, -1, k, a, b)
        send_y_row(s, -1)
        send_y_row(s, 1)
        ex = exchanges[2 * s + 1]
        ex.need(("r", -1), ("r", 1))
        if s == 1:
            for k, (a, b) in enumerate(zcuts[2]):
                need_y_col(s, -1, b)
                if k == 0:
                    ex.need(("d", 1, -1))
                if b == h:
                    ex.need(("d", -1, -1))
                conv(s, [(a, b)], 1, w)
                send_z_col(2, k, a, b)
            for k, (a, b) in enumerate(zcuts[2]):
                need_y_col(s, 1, b)
                if k == 0:
                    ex.need(("d", 1, 1))
                if b == h:
                    ex.need(("d", -1, 1))
                conv(s, [(a, b)], 0, 1)
            send_z_row(2)
        else:
            need_y_col(s, 1, h)
            need_y_col(s, -1, h)
            ex.need(*[("d", i, j) for i in (-1, 1) for j in (-1, 1)])
            conv(s, [(0, h)], 0, 1)
    for ex in exchanges:
        ex.finish()


def solution(mesh):
    row_count = mesh.shape["row"]
    col_count = mesh.shape["col"]
    tile_spec = P("batch", "row", "col")

    def local_blocks(x_tile, *params):
        images, tile_h, tile_w, c0 = x_tile.shape
        chans = [c0] + [params[5 * s].shape[-1] for s in range(3)]
        height = [tile_h >> s for s in range(4)]
        width = [tile_w >> s for s in range(4)]
        x_in = jnp.transpose(x_tile, (1, 2, 0, 3)).reshape(tile_h // 2, 2, tile_w // 2, 2, images, c0)
        operands, transposed, wshapes = [], [], []
        for s in range(3):
            for p in range(5):
                value = params[5 * s + p]
                if p in (1, 3):
                    operands.append(value.reshape(1, -1))
                    continue
                k, n = value.shape[-2:]
                flip = k % LANE == 0 and n % LANE != 0
                value = value.reshape(-1, k, n)
                if flip:
                    value = jnp.swapaxes(value, 1, 2)
                    wshapes.append(value.shape)
                else:
                    wshapes.append((value.shape[0], tiles_of(k) * LANE, n))
                operands.append(value)
                transposed.append(flip)
        zcut, ycut = (4, 3, 2), (4, 2, 1)
        cfg = dict(chans=chans, height=height, width=width, rows=row_count, cols=col_count, images=images, transposed=transposed, zcut=zcut, ycut=ycut)
        messages = sum(zcut) + 2 * 3 + 2 * sum(ycut) + 3 * 6
        bf16 = jnp.bfloat16
        scratch = [pltpu.VMEM((1, tile_h // 2 + 1, 2, tile_w // 2 + 1, 2, images, LANE), bf16)]
        for s in (1, 2, 3):
            scratch.append(pltpu.VMEM((tiles_of(chans[s]), height[s] + 2, width[s] + 2, images, LANE), bf16))
        for s in (1, 2):
            scratch.append(pltpu.VMEM((tiles_of(chans[s]), height[s] // 2 + 1, 2, width[s] // 2 + 1, 2, images, LANE), bf16))
        for shape in wshapes:
            scratch.append(pltpu.VMEM(shape, bf16))
        scratch += [pltpu.SemaphoreType.DMA((10,)), pltpu.SemaphoreType.DMA((2, messages))]
        hbm = pl.BlockSpec(memory_space=pl.ANY)
        vmem = pl.BlockSpec(memory_space=pltpu.VMEM)
        out = pl.pallas_call(
            functools.partial(body, cfg),
            out_shape=jax.ShapeDtypeStruct((height[3], images, chans[3]), bf16),
            in_specs=[hbm] + [vmem if p in (1, 3) else hbm for _ in range(3) for p in range(5)],
            out_specs=vmem,
            scratch_shapes=scratch,
            compiler_params=pltpu.CompilerParams(collective_id=0, has_side_effects=True, vmem_limit_bytes=60 * 1024 * 1024),
            name="encoder",
        )(x_in, *operands)
        return jnp.transpose(out, (1, 0, 2))[:, :, None, :]

    return jax.shard_map(local_blocks, mesh=mesh, in_specs=(tile_spec,) + (P(),) * 15, out_specs=tile_spec, check_vma=False)
```

```python
import functools

import jax
import jax.numpy as jnp
from jax import lax
from jax.experimental import pallas as pl
from jax.experimental.pallas import tpu as pltpu
from jax.sharding import PartitionSpec as P

LANE = 128
MESH = pl.DeviceIdType.MESH
NEIGHBOURS = [(dr, dc) for dr in (-1, 0, 1) for dc in (-1, 0, 1) if (dr, dc) != (0, 0)]


def tiles_of(channels):
    return -(-channels // LANE)


def cut(count, pieces, unit=1):
    bounds = [round(count * k / pieces / unit) * unit for k in range(pieces + 1)]
    return [(a, b) for a, b in zip(bounds, bounds[1:]) if b > a]


class Exchange:
    def __init__(self, grid, sems, counter):
        self.grid, self.sems, self.counter = grid, sems, counter
        self.copies = {}
        self.waited = set()

    def exists(self, dr, dc):
        row, col, row_count, col_count = self.grid
        tests = []
        if dr == 1:
            tests.append(row + 1 < row_count)
        if dr == -1:
            tests.append(row > 0)
        if dc == 1:
            tests.append(col + 1 < col_count)
        if dc == -1:
            tests.append(col > 0)
        return functools.reduce(jnp.logical_and, tests)

    def send(self, key, dr, dc, src, dst):
        row, col = self.grid[:2]
        index = self.counter[0]
        self.counter[0] += 1
        copy = pltpu.make_async_remote_copy(
            src_ref=src, dst_ref=dst, send_sem=self.sems.at[0, index], recv_sem=self.sems.at[1, index],
            device_id={"row": row + dr, "col": col + dc}, device_id_type=MESH)
        self.copies[key] = (copy, dr, dc)
        pl.when(self.exists(dr, dc))(copy.start)

    def need(self, *keys):
        for key in keys:
            if key not in self.waited:
                self.waited.add(key)
                copy, dr, dc = self.copies[key]
                pl.when(self.exists(-dr, -dc))(copy.wait_recv)

    def finish(self):
        assert self.waited == set(self.copies)
        for copy, dr, dc in self.copies.values():
            pl.when(self.exists(dr, dc))(copy.wait_send)


def body(cfg, x_hbm, *refs):
    params, refs = refs[:15], refs[15:]
    out_ref, raw, xs, ys, zs, ws, load_sems, sems = refs[0], refs[1], refs[2], refs[3:6], refs[6:8], refs[8:17], refs[17], refs[18]
    chans, height, width = cfg["chans"], cfg["height"], cfg["width"]
    row, col = lax.axis_index("row"), lax.axis_index("col")
    grid = (row, col, cfg["rows"], cfg["cols"])
    counter = [0]
    dtype = jnp.bfloat16
    images = cfg["images"]

    xcuts = cut(height[0], cfg["zcut"][0], 2)
    xloads = [pltpu.make_async_copy(x_hbm.at[:, a:b], raw.at[:, a:b], load_sems.at[9 + k]) for k, (a, b) in enumerate(xcuts)]
    loads = []
    for stage in range(3):
        for k, p in enumerate((0, 2, 4)):
            src, dst = params[5 * stage + p], ws[3 * stage + k]
            if dst.shape != src.shape:
                dst = dst.at[:, :src.shape[1]]
            loads.append(pltpu.make_async_copy(src, dst, load_sems.at[3 * stage + k]))
    for load in xloads + loads[:3]:
        load.start()

    def zero(ref):
        ref[...] = jnp.zeros(ref.shape, ref.dtype)

    for buf in (xs,) + tuple(zs):
        zero(buf.at[:, 0, 1])
        zero(buf.at[:, :, :, 0, 1])
    for buf in ys:
        zero(buf.at[:, 0:1])
        zero(buf.at[:, -1:])
        zero(buf.at[:, :, 0:1])
        zero(buf.at[:, :, -1:])
    for buf in tuple(ys[1:]) + tuple(zs[1:]):
        zero(buf.at[buf.shape[0] - 1:])
    for k, p in enumerate((0, 2, 4) * 3):
        src, dst = params[5 * (k // 3) + p], ws[k]
        if dst.shape != src.shape:
            zero(dst.at[:, src.shape[1]:])

    for load in loads[3:]:
        load.start()

    exchanges = [Exchange(grid, sems, counter) for _ in range(6)]
    barrier = pltpu.get_barrier_semaphore()
    for dr, dc in NEIGHBOURS:
        there = exchanges[0].exists(dr, dc)

        def greet(dr=dr, dc=dc):
            pl.semaphore_signal(barrier, inc=1, device_id={"row": row + dr, "col": col + dc}, device_id_type=MESH)

        pl.when(there)(greet)
    row_inner = jnp.logical_and(row > 0, row + 1 < cfg["rows"])
    col_inner = jnp.logical_and(col > 0, col + 1 < cfg["cols"])
    for row_peers, row_test in ((3, row_inner), (2, jnp.logical_not(row_inner))):
        for col_peers, col_test in ((3, col_inner), (2, jnp.logical_not(col_inner))):
            peers = row_peers * col_peers - 1
            pl.when(jnp.logical_and(row_test, col_test))(functools.partial(pl.semaphore_wait, barrier, peers))

    zin = [xs, zs[0], zs[1]]

    waited_loads = set()

    def wait_load(index):
        if index not in waited_loads:
            waited_loads.add(index)
            loads[index].wait()

    def flat(block):
        return block.reshape(-1, LANE)

    def stack(pieces):
        return pieces[0] if len(pieces) == 1 else jnp.concatenate(pieces, axis=0)

    def matrix(ref):
        value = ref[...]
        return value.reshape(-1, value.shape[-1])

    def times(lhs, ref, transposed):
        if transposed:
            return sum(lax.dot_general(lhs[:, t * ref.shape[2]:(t + 1) * ref.shape[2]], ref[t], (((1,), (1,)), ((), ())), preferred_element_type=jnp.float32)
                       for t in range(ref.shape[0]))
        return jnp.dot(lhs, matrix(ref), preferred_element_type=jnp.float32)

    def strided(src, ct, runs, kh, kw, c0, c1):
        up, lo = (1 if kh else 0), c0 + (1 if kw else 0)
        return stack([flat(src[ct, a + up:b + up, (kh + 1) % 2, lo:lo + c1 - c0, (kw + 1) % 2]) for a, b in runs])

    def centre(s, runs, c0, c1):
        src = zin[s]
        return jnp.concatenate([strided(src, ct, runs, 1, 1, c0, c1) for ct in range(src.shape[0])], axis=1)

    def down(s, rows, c0, c1):
        src, dst = zin[s], ys[s]
        wait_load(3 * s)
        taps = []
        for kh in range(3):
            for kw in range(3):
                for ct in range(src.shape[0]):
                    taps.append(strided(src, ct, rows, kh, kw, c0, c1))
        acc = times(jnp.concatenate(taps, axis=1), ws[3 * s], cfg["transposed"][3 * s])
        val = jnp.maximum(acc + params[5 * s + 1][...].reshape(1, -1), 0.0).astype(dtype)
        n = images * (c1 - c0)
        for ct in range(dst.shape[0]):
            l1 = min(chans[s + 1] - ct * LANE, LANE)
            r = 0
            for a, b in rows:
                part = val[r * n:(r + b - a) * n, ct * LANE:ct * LANE + l1]
                dst[ct, a + 1:b + 1, c0 + 1:c1 + 1, :, 0:l1] = part.reshape(b - a, c1 - c0, images, l1)
                r += b - a

    def conv(s, rows, c0, c1):
        src = ys[s]
        wait_load(3 * s + 1)
        wait_load(3 * s + 2)
        taps = []
        for kh in range(3):
            for kw in range(3):
                for ct in range(src.shape[0]):
                    taps.append(stack([flat(src[ct, a + kh:b + kh, c0 + kw:c1 + kw]) for a, b in rows]))
        acc = times(jnp.concatenate(taps, axis=1), ws[3 * s + 1], cfg["transposed"][3 * s + 1])
        acc += times(centre(s, rows, c0, c1), ws[3 * s + 2], cfg["transposed"][3 * s + 2])
        val = jnp.maximum(acc + params[5 * s + 3][...].reshape(1, -1), 0.0).astype(dtype)
        n = images * (c1 - c0)
        if s == 2:
            (a, b), = rows
            out_ref[a:b] = val.reshape(b - a, images, chans[3])
            return
        dst = zin[s + 1]
        for ct in range(dst.shape[0]):
            l1 = min(chans[s + 1] - ct * LANE, LANE)
            r = 0
            for a, b in rows:
                part = val[r * n:(r + b - a) * n, ct * LANE:ct * LANE + l1].reshape(b - a, c1 - c0, images, l1)
                r += b - a
                even, odd = a + a % 2, b - b % 2
                for c in range(c0, c1):
                    into = (c // 2 + 1, c % 2, slice(None), slice(0, l1))
                    if a < even:
                        dst[(ct, a // 2 + 1, 1) + into] = part[0, c - c0]
                    if odd > even:
                        dst[(ct, slice(even // 2 + 1, odd // 2 + 1), slice(None)) + into] = part[even - a:odd - a, c - c0].reshape((odd - even) // 2, 2, images, l1)
                    if odd < b and b - 1 >= even:
                        dst[(ct, odd // 2 + 1, 0) + into] = part[b - 1 - a, c - c0]

    def send_y_col(s, side, k, a, b):
        y, w = ys[s], width[s + 1]
        own, there = (w, 0) if side > 0 else (1, w + 1)
        exchanges[2 * s + 1].send(("c", side, k), 0, side, y.at[:, 1 + a:1 + b, own], y.at[:, 1 + a:1 + b, there])

    def send_y_row(s, side):
        y, h, w = ys[s], height[s + 1], width[s + 1]
        own, there = (h, 0) if side > 0 else (1, h + 1)
        ex = exchanges[2 * s + 1]
        ex.send(("r", side), side, 0, y.at[:, own, 1:w + 1], y.at[:, there, 1:w + 1])
        ex.send(("d", side, 1), side, 1, y.at[:, own, w], y.at[:, there, 0])
        ex.send(("d", side, -1), side, -1, y.at[:, own, 1], y.at[:, there, w + 1])

    def send_z_col(s, k, a, b):
        z, w = zin[s], width[s]
        exchanges[2 * s].send(("c", k), 0, 1, z.at[:, 1 + a // 2:1 + b // 2, :, w // 2, 1], z.at[:, 1 + a // 2:1 + b // 2, :, 0, 1])

    def send_z_row(s):
        z, h, w = zin[s], height[s], width[s]
        ex = exchanges[2 * s]
        ex.send("r", 1, 0, z.at[:, h // 2, 1, 1:], z.at[:, 0, 1, 1:])
        ex.send("d", 1, 1, z.at[:, h // 2, 1, w // 2, 1], z.at[:, 0, 1, 0, 1])

    def need_z_col(s, b):
        for k, (lo, hi) in enumerate(zcuts[s]):
            if lo < 2 * b:
                exchanges[2 * s].need(("c", k))

    def need_y_col(s, side, b):
        for k, (lo, hi) in enumerate(ycuts[s]):
            if lo < b + 1:
                exchanges[2 * s + 1].need(("c", side, k))

    def blocks(lo, hi, size):
        return [[(k, min(k + size, hi))] for k in range(lo, hi, size)]

    zcuts = [cut(height[s], cfg["zcut"][s], 2) for s in range(3)]
    ycuts = [cut(height[s + 1], cfg["ycut"][s]) for s in range(3)]

    for k, (a, b) in enumerate(zcuts[0]):
        xloads[k].wait()
        for i in range(a, b):
            tile = jnp.swapaxes(raw[:, i], 0, 1)
            xs[0, i // 2 + 1, i % 2, 1:] = tile.reshape(width[0] // 2, 2, images, LANE)
        send_z_col(0, k, a, b)
    send_z_row(0)
    ex = exchanges[0]

    h1, w1 = height[1], width[1]
    for rows in blocks(8, h1, 8):
        down(0, rows, 1, w1)
    ex.need("r")
    down(0, [(0, 8)], 1, w1)
    for k, (a, b) in enumerate(ycuts[0]):
        send_y_col(0, 1, k, a, b)
    for k, (a, b) in enumerate(ycuts[0]):
        need_z_col(0, b)
        if k == 0:
            ex.need("d")
        down(0, [(a, b)], 0, 1)
        send_y_col(0, -1, k, a, b)
        if k == 0:
            send_y_row(0, -1)
        if b == h1:
            send_y_row(0, 1)
        lo, hi = max(a - 1, 1), b - 1
        for rows in blocks(lo, hi, 8):
            conv(0, rows, 1, w1 - 1)
    ex = exchanges[1]
    ex.need(("r", -1), ("r", 1))
    conv(0, [(0, 1), (h1 - 1, h1)], 1, w1 - 1)
    for k, (a, b) in enumerate(zcuts[1]):
        need_y_col(0, -1, b)
        if k == 0:
            ex.need(("d", 1, -1))
        if b == h1:
            ex.need(("d", -1, -1))
        conv(0, [(a, b)], w1 - 1, w1)
        send_z_col(1, k, a, b)
    for k, (a, b) in enumerate(zcuts[1]):
        need_y_col(0, 1, b)
        if k == 0:
            ex.need(("d", 1, 1))
        if b == h1:
            ex.need(("d", -1, 1))
        conv(0, [(a, b)], 0, 1)
    send_z_row(1)

    for s in (1, 2):
        h, w = height[s + 1], width[s + 1]
        ex = exchanges[2 * s]
        ex.need("r")
        if w > 1:
            for rows in blocks(0, h, 12):
                down(s, rows, 1, w)
            for k, (a, b) in enumerate(ycuts[s]):
                send_y_col(s, 1, k, a, b)
        for k, (a, b) in enumerate(ycuts[s]):
            need_z_col(s, b)
            if k == 0:
                ex.need("d")
            down(s, [(a, b)], 0, 1)
            if w == 1:
                send_y_col(s, 1, k, a, b)
            send_y_col(s, -1, k, a, b)
        send_y_row(s, -1)
        send_y_row(s, 1)
        ex = exchanges[2 * s + 1]
        ex.need(("r", -1), ("r", 1))
        if s == 1:
            for k, (a, b) in enumerate(zcuts[2]):
                need_y_col(s, -1, b)
                if k == 0:
                    ex.need(("d", 1, -1))
                if b == h:
                    ex.need(("d", -1, -1))
                conv(s, [(a, b)], 1, w)
                send_z_col(2, k, a, b)
            for k, (a, b) in enumerate(zcuts[2]):
                need_y_col(s, 1, b)
                if k == 0:
                    ex.need(("d", 1, 1))
                if b == h:
                    ex.need(("d", -1, 1))
                conv(s, [(a, b)], 0, 1)
            send_z_row(2)
        else:
            need_y_col(s, 1, h)
            need_y_col(s, -1, h)
            ex.need(*[("d", i, j) for i in (-1, 1) for j in (-1, 1)])
            conv(s, [(0, h)], 0, 1)
    for ex in exchanges:
        ex.finish()


def solution(mesh):
    row_count = mesh.shape["row"]
    col_count = mesh.shape["col"]
    tile_spec = P("batch", "row", "col")

    def local_blocks(x_tile, *params):
        images, tile_h, tile_w, c0 = x_tile.shape
        chans = [c0] + [params[5 * s].shape[-1] for s in range(3)]
        height = [tile_h >> s for s in range(4)]
        width = [tile_w >> s for s in range(4)]
        operands, transposed, wshapes = [], [], []
        for s in range(3):
            for p in range(5):
                value = params[5 * s + p]
                if p in (1, 3):
                    operands.append(value)
                    continue
                k, n = value.shape[-2:]
                flip = k % LANE == 0 and n % LANE != 0
                value = value.reshape(-1, k, n)
                if flip:
                    value = jnp.swapaxes(value, 1, 2)
                    wshapes.append(value.shape)
                else:
                    wshapes.append((value.shape[0], tiles_of(k) * LANE, n))
                operands.append(value)
                transposed.append(flip)
        zcut, ycut = (4, 3, 2), (4, 2, 1)
        cfg = dict(chans=chans, height=height, width=width, rows=row_count, cols=col_count, images=images, transposed=transposed, zcut=zcut, ycut=ycut)
        messages = sum(zcut) + 2 * 3 + 2 * sum(ycut) + 3 * 6
        bf16 = jnp.bfloat16
        scratch = [pltpu.VMEM(x_tile.shape, bf16), pltpu.VMEM((1, tile_h // 2 + 1, 2, tile_w // 2 + 1, 2, images, LANE), bf16)]
        for s in (1, 2, 3):
            scratch.append(pltpu.VMEM((tiles_of(chans[s]), height[s] + 2, width[s] + 2, images, LANE), bf16))
        for s in (1, 2):
            scratch.append(pltpu.VMEM((tiles_of(chans[s]), height[s] // 2 + 1, 2, width[s] // 2 + 1, 2, images, LANE), bf16))
        for shape in wshapes:
            scratch.append(pltpu.VMEM(shape, bf16))
        scratch += [pltpu.SemaphoreType.DMA((9 + zcut[0],)), pltpu.SemaphoreType.DMA((2, messages))]
        hbm = pl.BlockSpec(memory_space=pl.ANY)
        vmem = pl.BlockSpec(memory_space=pltpu.VMEM)
        out = pl.pallas_call(
            functools.partial(body, cfg),
            out_shape=jax.ShapeDtypeStruct((height[3], images, chans[3]), bf16),
            in_specs=[hbm] + [vmem if p in (1, 3) else hbm for _ in range(3) for p in range(5)],
            out_specs=vmem,
            scratch_shapes=scratch,
            compiler_params=pltpu.CompilerParams(collective_id=0, has_side_effects=True, vmem_limit_bytes=60 * 1024 * 1024),
            name="encoder",
        )(x_tile, *operands)
        return jnp.transpose(out, (1, 0, 2))[:, :, None, :]

    return jax.shard_map(local_blocks, mesh=mesh, in_specs=(tile_spec,) + (P(),) * 15, out_specs=tile_spec, check_vma=False)
```

```python
import functools

import jax
import jax.numpy as jnp
from jax import lax
from jax.experimental import pallas as pl
from jax.experimental.pallas import tpu as pltpu
from jax.sharding import PartitionSpec as P

LANE = 128
MESH = pl.DeviceIdType.MESH
NEIGHBOURS = [(dr, dc) for dr in (-1, 0, 1) for dc in (-1, 0, 1) if (dr, dc) != (0, 0)]


def tiles_of(channels):
    return -(-channels // LANE)


def cut(count, pieces, unit=1):
    bounds = [round(count * k / pieces / unit) * unit for k in range(pieces + 1)]
    return [(a, b) for a, b in zip(bounds, bounds[1:]) if b > a]


class Exchange:
    def __init__(self, grid, sems, counter):
        self.grid, self.sems, self.counter = grid, sems, counter
        self.copies = {}
        self.waited = set()

    def exists(self, dr, dc):
        row, col, row_count, col_count = self.grid
        tests = []
        if dr == 1:
            tests.append(row + 1 < row_count)
        if dr == -1:
            tests.append(row > 0)
        if dc == 1:
            tests.append(col + 1 < col_count)
        if dc == -1:
            tests.append(col > 0)
        return functools.reduce(jnp.logical_and, tests)

    def send(self, key, dr, dc, src, dst):
        row, col = self.grid[:2]
        index = self.counter[0]
        self.counter[0] += 1
        copy = pltpu.make_async_remote_copy(
            src_ref=src, dst_ref=dst, send_sem=self.sems.at[0, index], recv_sem=self.sems.at[1, index],
            device_id={"row": row + dr, "col": col + dc}, device_id_type=MESH)
        self.copies[key] = (copy, dr, dc)
        pl.when(self.exists(dr, dc))(copy.start)

    def need(self, *keys):
        for key in keys:
            if key not in self.waited:
                self.waited.add(key)
                copy, dr, dc = self.copies[key]
                pl.when(self.exists(-dr, -dc))(copy.wait_recv)

    def finish(self):
        assert self.waited == set(self.copies)
        for copy, dr, dc in self.copies.values():
            pl.when(self.exists(dr, dc))(copy.wait_send)


def body(cfg, x_hbm, *refs):
    params, refs = refs[:15], refs[15:]
    out_ref, raw, xs, ys, zs, ws, load_sems, sems = refs[0], refs[1], refs[2], refs[3:6], refs[6:8], refs[8:17], refs[20], refs[21]
    packs = refs[17:20]
    packs = (packs[1], packs[0], None, packs[2])
    chans, height, width = cfg["chans"], cfg["height"], cfg["width"]
    row, col = lax.axis_index("row"), lax.axis_index("col")
    grid = (row, col, cfg["rows"], cfg["cols"])
    counter = [0]
    dtype = jnp.bfloat16
    images = cfg["images"]

    xcuts = cut(height[0], cfg["zcut"][0], 2)
    xloads = [pltpu.make_async_copy(x_hbm.at[:, a:b], raw.at[:, a:b], load_sems.at[9 + k]) for k, (a, b) in enumerate(xcuts)]
    loads = []
    for stage in range(3):
        for k, p in enumerate((0, 2, 4)):
            src, dst = params[5 * stage + p], ws[3 * stage + k]
            if dst.shape != src.shape:
                dst = dst.at[:, :src.shape[1]]
            loads.append(pltpu.make_async_copy(src, dst, load_sems.at[3 * stage + k]))
    for load in xloads + loads[:3]:
        load.start()

    def zero(ref):
        ref[...] = jnp.zeros(ref.shape, ref.dtype)

    for buf in (xs,) + tuple(zs):
        zero(buf.at[:, 0, 1])
        zero(buf.at[:, :, :, 0, 1])
    for buf in ys:
        zero(buf.at[:, 0:1])
        zero(buf.at[:, -1:])
        zero(buf.at[:, :, 0:1])
        zero(buf.at[:, :, -1:])
    for buf in tuple(ys[1:]) + tuple(zs[1:]):
        zero(buf.at[buf.shape[0] - 1:])
    for k, p in enumerate((0, 2, 4) * 3):
        src, dst = params[5 * (k // 3) + p], ws[k]
        if dst.shape != src.shape:
            zero(dst.at[:, src.shape[1]:])

    for load in loads[3:]:
        load.start()

    exchanges = [Exchange(grid, sems, counter) for _ in range(6)]
    barrier = pltpu.get_barrier_semaphore()
    for dr, dc in NEIGHBOURS:
        there = exchanges[0].exists(dr, dc)

        def greet(dr=dr, dc=dc):
            pl.semaphore_signal(barrier, inc=1, device_id={"row": row + dr, "col": col + dc}, device_id_type=MESH)

        pl.when(there)(greet)
    zin = [xs, zs[0], zs[1]]

    waited_loads = set()

    def wait_load(index):
        if index not in waited_loads:
            waited_loads.add(index)
            loads[index].wait()

    def flat(block):
        return block.reshape(-1, LANE)

    def stack(pieces):
        return pieces[0] if len(pieces) == 1 else jnp.concatenate(pieces, axis=0)

    def matrix(ref):
        value = ref[...]
        return value.reshape(-1, value.shape[-1])

    def times(lhs, ref, transposed):
        if transposed:
            return sum(lax.dot_general(lhs[:, t * ref.shape[2]:(t + 1) * ref.shape[2]], ref[t], (((1,), (1,)), ((), ())), preferred_element_type=jnp.float32)
                       for t in range(ref.shape[0]))
        return jnp.dot(lhs, matrix(ref), preferred_element_type=jnp.float32)

    def strided(src, ct, runs, kh, kw, c0, c1):
        up, lo = (1 if kh else 0), c0 + (1 if kw else 0)
        return stack([flat(src[ct, a + up:b + up, (kh + 1) % 2, lo:lo + c1 - c0, (kw + 1) % 2]) for a, b in runs])

    def centre(s, runs, c0, c1):
        src = zin[s]
        return jnp.concatenate([strided(src, ct, runs, 1, 1, c0, c1) for ct in range(src.shape[0])], axis=1)

    def down(s, rows, c0, c1):
        src, dst = zin[s], ys[s]
        wait_load(3 * s)
        taps = []
        for kh in range(3):
            for kw in range(3):
                for ct in range(src.shape[0]):
                    taps.append(strided(src, ct, rows, kh, kw, c0, c1))
        acc = times(jnp.concatenate(taps, axis=1), ws[3 * s], cfg["transposed"][3 * s])
        val = jnp.maximum(acc + params[5 * s + 1][...].reshape(1, -1), 0.0).astype(dtype)
        n = images * (c1 - c0)
        for ct in range(dst.shape[0]):
            l1 = min(chans[s + 1] - ct * LANE, LANE)
            r = 0
            for a, b in rows:
                part = val[r * n:(r + b - a) * n, ct * LANE:ct * LANE + l1]
                dst[ct, a + 1:b + 1, c0 + 1:c1 + 1, :, 0:l1] = part.reshape(b - a, c1 - c0, images, l1)
                r += b - a

    def conv(s, rows, c0, c1):
        src = ys[s]
        wait_load(3 * s + 1)
        wait_load(3 * s + 2)
        taps = []
        for kh in range(3):
            for kw in range(3):
                for ct in range(src.shape[0]):
                    taps.append(stack([flat(src[ct, a + kh:b + kh, c0 + kw:c1 + kw]) for a, b in rows]))
        acc = times(jnp.concatenate(taps, axis=1), ws[3 * s + 1], cfg["transposed"][3 * s + 1])
        acc += times(centre(s, rows, c0, c1), ws[3 * s + 2], cfg["transposed"][3 * s + 2])
        val = jnp.maximum(acc + params[5 * s + 3][...].reshape(1, -1), 0.0).astype(dtype)
        n = images * (c1 - c0)
        if s == 2:
            (a, b), = rows
            out_ref[a:b] = val.reshape(b - a, images, chans[3])
            return
        dst = zin[s + 1]
        for ct in range(dst.shape[0]):
            l1 = min(chans[s + 1] - ct * LANE, LANE)
            r = 0
            for a, b in rows:
                part = val[r * n:(r + b - a) * n, ct * LANE:ct * LANE + l1].reshape(b - a, c1 - c0, images, l1)
                r += b - a
                even, odd = a + a % 2, b - b % 2
                for c in range(c0, c1):
                    into = (c // 2 + 1, c % 2, slice(None), slice(0, l1))
                    if a < even:
                        dst[(ct, a // 2 + 1, 1) + into] = part[0, c - c0]
                    if odd > even:
                        dst[(ct, slice(even // 2 + 1, odd // 2 + 1), slice(None)) + into] = part[even - a:odd - a, c - c0].reshape((odd - even) // 2, 2, images, l1)
                    if odd < b and b - 1 >= even:
                        dst[(ct, odd // 2 + 1, 0) + into] = part[b - 1 - a, c - c0]

    def halves(tile):
        return pltpu.roll(tile.astype(jnp.float32), LANE // 2, tile.ndim - 1).astype(dtype)

    lower = lax.broadcasted_iota(jnp.int32, (1, images, LANE), 2) < LANE // 2

    def send_column(ex, key, side, buf, packed, own, there, count, k):
        full = buf.shape[0] if packed is None else buf.shape[0] - 1
        ex.send(key, 0, side, own(slice(0, full)), there(slice(0, full)))
        if packed is not None:
            out, into = packed
            rest = own(full)[...].reshape(count // 2, 2, images, LANE)
            out[...] = jnp.where(lower, rest[:, 0], halves(rest[:, 1]))
            ex.send(key + ("rest",), 0, side, out, into)

    def unpack(into, packed, count):
        tile = packed[1][...]
        none = jnp.zeros_like(tile)
        rest = jnp.stack([jnp.where(lower, tile, none), jnp.where(lower, halves(tile), none)], axis=1)
        into[...] = rest.reshape(into.shape)

    def need_column(ex, key, side, into, packed, count):
        if key in ex.waited:
            return
        ex.need(key)
        if packed is not None:
            ex.need(key + ("rest",))
            pl.when(ex.exists(0, -side))(functools.partial(unpack, into, packed, count))

    def y_packed(s, side, a, b):
        if s == 0:
            return None
        at = 0 if side > 0 else 1
        return packs[2 * s - 1].at[0, at, a // 2:b // 2], packs[2 * s - 1].at[1, at, a // 2:b // 2]

    def z_packed(s, a, b):
        if s < 2:
            return None
        return packs[0].at[0, a // 2:b // 2], packs[0].at[1, a // 2:b // 2]

    def send_y_col(s, side, k, a, b):
        y, w = ys[s], width[s + 1]
        own, there = (w, 0) if side > 0 else (1, w + 1)
        send_column(exchanges[2 * s + 1], ("c", side, k), side, y, y_packed(s, side, a, b),
                    lambda ct: y.at[ct, 1 + a:1 + b, own], lambda ct: y.at[ct, 1 + a:1 + b, there], b - a, k)

    def send_y_row(s, side):
        y, h, w = ys[s], height[s + 1], width[s + 1]
        own, there = (h, 0) if side > 0 else (1, h + 1)
        ex = exchanges[2 * s + 1]
        ex.send(("r", side), side, 0, y.at[:, own, 1:w + 1], y.at[:, there, 1:w + 1])
        ex.send(("d", side, 1), side, 1, y.at[:, own, w], y.at[:, there, 0])
        ex.send(("d", side, -1), side, -1, y.at[:, own, 1], y.at[:, there, w + 1])

    def send_z_col(s, k, a, b):
        z, w = zin[s], width[s]
        rows = slice(1 + a // 2, 1 + b // 2)
        send_column(exchanges[2 * s], ("c", k), 1, z, z_packed(s, a, b),
                    lambda ct: z.at[ct, rows, :, w // 2, 1], lambda ct: z.at[ct, rows, :, 0, 1], b - a, k)

    def send_z_row(s):
        z, h, w = zin[s], height[s], width[s]
        ex = exchanges[2 * s]
        ex.send("r", 1, 0, z.at[:, h // 2, 1, 1:], z.at[:, 0, 1, 1:])
        ex.send("d", 1, 1, z.at[:, h // 2, 1, w // 2, 1], z.at[:, 0, 1, 0, 1])

    def need_z_col(s, b):
        for k, (lo, hi) in enumerate(zcuts[s]):
            if lo < 2 * b:
                z = zin[s]
                need_column(exchanges[2 * s], ("c", k), 1, z.at[z.shape[0] - 1, 1 + lo // 2:1 + hi // 2, :, 0, 1], z_packed(s, lo, hi), hi - lo)

    def need_y_col(s, side, b):
        for k, (lo, hi) in enumerate(ycuts[s]):
            if lo < b + 1:
                y = ys[s]
                need_column(exchanges[2 * s + 1], ("c", side, k), side, y.at[y.shape[0] - 1, 1 + lo:1 + hi, 0 if side > 0 else width[s + 1] + 1], y_packed(s, side, lo, hi), hi - lo)

    def blocks(lo, hi, size):
        return [[(k, min(k + size, hi))] for k in range(lo, hi, size)]

    zcuts = [cut(height[s], cfg["zcut"][s], 2) for s in range(3)]
    ycuts = [cut(height[s + 1], cfg["ycut"][s], 2) for s in range(3)]

    for k, (a, b) in enumerate(zcuts[0]):
        xloads[k].wait()
        for i in range(a, b):
            tile = jnp.swapaxes(raw[:, i], 0, 1)
            xs[0, i // 2 + 1, i % 2, 1:] = tile.reshape(width[0] // 2, 2, images, LANE)

    row_inner = jnp.logical_and(row > 0, row + 1 < cfg["rows"])
    col_inner = jnp.logical_and(col > 0, col + 1 < cfg["cols"])
    for row_peers, row_test in ((3, row_inner), (2, jnp.logical_not(row_inner))):
        for col_peers, col_test in ((3, col_inner), (2, jnp.logical_not(col_inner))):
            peers = row_peers * col_peers - 1
            pl.when(jnp.logical_and(row_test, col_test))(functools.partial(pl.semaphore_wait, barrier, peers))

    for k, (a, b) in enumerate(zcuts[0]):
        send_z_col(0, k, a, b)
    send_z_row(0)
    ex = exchanges[0]

    h1, w1 = height[1], width[1]
    for rows in blocks(8, h1, 8):
        down(0, rows, 1, w1)
    ex.need("r")
    down(0, [(0, 8)], 1, w1)
    for k, (a, b) in enumerate(ycuts[0]):
        send_y_col(0, 1, k, a, b)
    for k, (a, b) in enumerate(ycuts[0]):
        need_z_col(0, b)
        if k == 0:
            ex.need("d")
        down(0, [(a, b)], 0, 1)
        send_y_col(0, -1, k, a, b)
        if k == 0:
            send_y_row(0, -1)
        if b == h1:
            send_y_row(0, 1)
        lo, hi = max(a - 1, 1), b - 1
        for rows in blocks(lo, hi, 8):
            conv(0, rows, 1, w1 - 1)
    ex = exchanges[1]
    ex.need(("r", -1), ("r", 1))
    conv(0, [(0, 1), (h1 - 1, h1)], 1, w1 - 1)
    for k, (a, b) in enumerate(zcuts[1]):
        need_y_col(0, -1, b)
        if k == 0:
            ex.need(("d", 1, -1))
        if b == h1:
            ex.need(("d", -1, -1))
        conv(0, [(a, b)], w1 - 1, w1)
        send_z_col(1, k, a, b)
    for k, (a, b) in enumerate(zcuts[1]):
        need_y_col(0, 1, b)
        if k == 0:
            ex.need(("d", 1, 1))
        if b == h1:
            ex.need(("d", -1, 1))
        conv(0, [(a, b)], 0, 1)
    send_z_row(1)

    for s in (1, 2):
        h, w = height[s + 1], width[s + 1]
        ex = exchanges[2 * s]
        ex.need("r")
        if w > 1:
            for rows in blocks(0, h, 12):
                down(s, rows, 1, w)
        for k, (a, b) in enumerate(ycuts[s]):
            need_z_col(s, b)
            if k == 0:
                ex.need("d")
            down(s, [(a, b)], 0, 1)
            send_y_col(s, -1, k, a, b)
            send_y_col(s, 1, k, a, b)
        send_y_row(s, -1)
        send_y_row(s, 1)
        ex = exchanges[2 * s + 1]
        ex.need(("r", -1), ("r", 1))
        if s == 1:
            for k, (a, b) in enumerate(zcuts[2]):
                need_y_col(s, -1, b)
                if k == 0:
                    ex.need(("d", 1, -1))
                if b == h:
                    ex.need(("d", -1, -1))
                conv(s, [(a, b)], 1, w)
                send_z_col(2, k, a, b)
            for k, (a, b) in enumerate(zcuts[2]):
                need_y_col(s, 1, b)
                if k == 0:
                    ex.need(("d", 1, 1))
                if b == h:
                    ex.need(("d", -1, 1))
                conv(s, [(a, b)], 0, 1)
            send_z_row(2)
        else:
            need_y_col(s, 1, h)
            need_y_col(s, -1, h)
            ex.need(*[("d", i, j) for i in (-1, 1) for j in (-1, 1)])
            conv(s, [(0, h)], 0, 1)
    for ex in exchanges:
        ex.finish()


def solution(mesh):
    row_count = mesh.shape["row"]
    col_count = mesh.shape["col"]
    tile_spec = P("batch", "row", "col")

    def local_blocks(x_tile, *params):
        images, tile_h, tile_w, c0 = x_tile.shape
        chans = [c0] + [params[5 * s].shape[-1] for s in range(3)]
        height = [tile_h >> s for s in range(4)]
        width = [tile_w >> s for s in range(4)]
        operands, transposed, wshapes = [], [], []
        for s in range(3):
            for p in range(5):
                value = params[5 * s + p]
                if p in (1, 3):
                    operands.append(value)
                    continue
                k, n = value.shape[-2:]
                flip = k % LANE == 0 and n % LANE != 0
                value = value.reshape(-1, k, n)
                if flip:
                    value = jnp.swapaxes(value, 1, 2)
                    wshapes.append(value.shape)
                else:
                    wshapes.append((value.shape[0], tiles_of(k) * LANE, n))
                operands.append(value)
                transposed.append(flip)
        zcut, ycut = (4, 3, 2), (4, 2, 1)
        cfg = dict(chans=chans, height=height, width=width, rows=row_count, cols=col_count, images=images, transposed=transposed, zcut=zcut, ycut=ycut)
        messages = 2 * sum(zcut) + 2 * 3 + 4 * sum(ycut) + 3 * 6
        bf16 = jnp.bfloat16
        scratch = [pltpu.VMEM(x_tile.shape, bf16), pltpu.VMEM((1, tile_h // 2 + 1, 2, tile_w // 2 + 1, 2, images, LANE), bf16)]
        for s in (1, 2, 3):
            scratch.append(pltpu.VMEM((tiles_of(chans[s]), height[s] + 2, width[s] + 2, images, LANE), bf16))
        for s in (1, 2):
            scratch.append(pltpu.VMEM((tiles_of(chans[s]), height[s] // 2 + 1, 2, width[s] // 2 + 1, 2, images, LANE), bf16))
        for shape in wshapes:
            scratch.append(pltpu.VMEM(shape, bf16))
        scratch.append(pltpu.VMEM((2, 2, height[2] // 2, images, LANE), bf16))
        scratch.append(pltpu.VMEM((2, height[2] // 2, images, LANE), bf16))
        scratch.append(pltpu.VMEM((2, 2, height[3] // 2, images, LANE), bf16))
        scratch += [pltpu.SemaphoreType.DMA((9 + zcut[0],)), pltpu.SemaphoreType.DMA((2, messages))]
        hbm = pl.BlockSpec(memory_space=pl.ANY)
        vmem = pl.BlockSpec(memory_space=pltpu.VMEM)
        out = pl.pallas_call(
            functools.partial(body, cfg),
            out_shape=jax.ShapeDtypeStruct((height[3], images, chans[3]), bf16),
            in_specs=[hbm] + [vmem if p in (1, 3) else hbm for _ in range(3) for p in range(5)],
            out_specs=vmem,
            scratch_shapes=scratch,
            compiler_params=pltpu.CompilerParams(collective_id=0, has_side_effects=True, vmem_limit_bytes=60 * 1024 * 1024),
            name="encoder",
        )(x_tile, *operands)
        return jnp.transpose(out, (1, 0, 2))[:, :, None, :]

    return jax.shard_map(local_blocks, mesh=mesh, in_specs=(tile_spec,) + (P(),) * 15, out_specs=tile_spec, check_vma=False)
```

```python
import functools

import jax
import jax.numpy as jnp
from jax import lax
from jax.experimental import pallas as pl
from jax.experimental.pallas import tpu as pltpu
from jax.sharding import PartitionSpec as P

LANE = 128
MESH = pl.DeviceIdType.MESH
NEIGHBOURS = [(dr, dc) for dr in range(-1, 2) for dc in range(-1, 2) if dr or dc]


def tiles_of(channels):
    return -(-channels // LANE)


def cut(count, pieces, unit=1):
    bounds = [round(count * k / pieces / unit) * unit for k in range(pieces + 1)]
    return [(a, b) for a, b in zip(bounds, bounds[1:]) if b > a]


WEIGHTS = (0, 2, 4)
PACKS = [("y", s, name) for s in range(1, 3) for name in ("left", "right")] + [("z", 2, "left")]


class Exchange:
    def __init__(self, grid, sems, counter, known):
        self.grid, self.sems, self.counter = grid, sems, counter
        self.copies = {}
        self.known = known
        self.landing = {}
        self.waited = set()

    def exists(self, dr, dc):
        if (dr, dc) not in self.known:
            row, col, row_count, col_count = self.grid
            tests = []
            if dr:
                tests.append(row + 1 < row_count if dr > 0 else row > 0)
            if dc:
                tests.append(col + 1 < col_count if dc > 0 else col > 0)
            self.known[dr, dc] = functools.reduce(jnp.logical_and, tests)
        return self.known[dr, dc]

    def arrives(self, key):
        dr, dc = self.copies[key][1:]
        return self.exists(-dr, -dc)

    def send(self, key, dr, dc, src, dst, before=None, then=None):
        row, col = self.grid[:2]
        copies = []
        for name, source, target in ((key, src, dst),) + (then or ()):
            index = self.counter[0]
            self.counter[0] += 1
            copy = pltpu.make_async_remote_copy(
                src_ref=source, dst_ref=target, send_sem=self.sems.at[0, index], recv_sem=self.sems.at[1, index],
                device_id={"row": row + dr, "col": col + dc}, device_id_type=MESH)
            self.copies[name] = (copy, dr, dc)
            copies.append(copy)

        def start():
            copies[0].start()
            if before is not None:
                before()
            for copy in copies[1:]:
                copy.start()

        pl.when(self.exists(dr, dc))(start)

    def together(self, groups):
        for test, waits in groups:
            def wait(waits=waits):
                for one in waits:
                    one()

            pl.when(test)(wait)

    def need(self, *keys, after=None):
        groups = {}
        for key in keys:
            if key not in self.waited:
                self.waited.add(key)
                test = self.arrives(key)
                groups.setdefault(id(test), (test, []))[1].append(self.copies[key][0].wait_recv)
        if after is not None:
            for test, waits in groups.values():
                waits.append(after)
        self.together(groups.values())

    def sends(self):
        assert self.waited == set(self.copies)
        return [(self.exists(dr, dc), copy.wait_send) for copy, dr, dc in self.copies.values()]


def body(cfg, x_hbm, *refs):
    params, refs = refs[:15], refs[15:]
    out_ref, raw, xs, y1, y2, y3, z1, z2, *ws, packs, load_sems, sems = refs
    ys, zs = (y1, y2, y3), (z1, z2)
    chans, height, width = cfg["chans"], cfg["height"], cfg["width"]
    row, col = lax.axis_index("row"), lax.axis_index("col")
    grid = (row, col, cfg["rows"], cfg["cols"])
    counter = [0]
    known = {}
    dtype = jnp.bfloat16
    images = cfg["images"]

    xcuts = cut(height[0], cfg["zcut"][0], 2)
    xloads = [pltpu.make_async_copy(x_hbm.at[:, a:b], raw.at[:, a:b], load_sems.at[9 + k]) for k, (a, b) in enumerate(xcuts)]
    loads = []
    for stage in range(3):
        for k, p in enumerate(WEIGHTS):
            src, dst = params[5 * stage + p], ws[3 * stage + k]
            if dst.shape != src.shape:
                dst = dst.at[:, :src.shape[1]]
            loads.append(pltpu.make_async_copy(src, dst, load_sems.at[3 * stage + k]))
    for load in xloads + loads[:3]:
        load.start()

    def zero(ref):
        ref[...] = jnp.zeros(ref.shape, ref.dtype)

    for buf in (xs,) + tuple(zs):
        zero(buf.at[:, 0, 1])
        zero(buf.at[:, :, :, 0, 1])
    for s, buf in enumerate(ys):
        zero(buf.at[:, 0:1])
        zero(buf.at[:, -1:])
        zero(buf.at[:, :, 0:1])
        zero(buf.at[:, :, width[s + 1] + 1:])
    for buf in tuple(ys[1:]) + tuple(zs[1:]):
        zero(buf.at[buf.shape[0] - 1:])
    for k, p in enumerate(WEIGHTS * 3):
        src, dst = params[5 * (k // 3) + p], ws[k]
        if dst.shape != src.shape:
            zero(dst.at[:, src.shape[1]:])

    for load in loads[3:]:
        load.start()

    exchanges = [Exchange(grid, sems, counter, known) for _ in range(6)]
    barrier = pltpu.get_barrier_semaphore()
    for dr, dc in NEIGHBOURS:
        there = exchanges[0].exists(dr, dc)

        def greet(dr=dr, dc=dc):
            pl.semaphore_signal(barrier, inc=1, device_id={"row": row + dr, "col": col + dc}, device_id_type=MESH)

        pl.when(there)(greet)
    zin = [xs, zs[0], zs[1]]

    waited_loads = set()

    def wait_load(index):
        if index not in waited_loads:
            waited_loads.add(index)
            loads[index].wait()

    def flat(block):
        return block.reshape(-1, LANE)

    def stack(pieces):
        return pieces[0] if len(pieces) == 1 else jnp.concatenate(pieces, axis=0)

    def matrix(ref):
        value = ref[...]
        return value.reshape(-1, value.shape[-1])

    def times(lhs, ref, transposed):
        if transposed:
            return sum(lax.dot_general(lhs[:, t * ref.shape[2]:(t + 1) * ref.shape[2]], ref[t], (((1,), (1,)), ((), ())), preferred_element_type=jnp.float32)
                       for t in range(ref.shape[0]))
        return jnp.dot(lhs, matrix(ref), preferred_element_type=jnp.float32)

    def strided(src, ct, runs, kh, kw, c0, nc):
        up, lo = (1 if kh else 0), c0 + (1 if kw else 0)
        return stack([flat(src[ct, a + up:b + up, (kh + 1) % 2, pl.ds(lo, nc), (kw + 1) % 2]) for a, b in runs])

    def centre(s, runs, c0, nc):
        src = zin[s]
        return jnp.concatenate([strided(src, ct, runs, 1, 1, c0, nc) for ct in range(src.shape[0])], axis=1)

    def down(s, rows, c0, nc=1):
        src, dst = zin[s], ys[s]
        wait_load(3 * s)
        taps = []
        for kh in range(3):
            for kw in range(3):
                for ct in range(src.shape[0]):
                    taps.append(strided(src, ct, rows, kh, kw, c0, nc))
        acc = times(jnp.concatenate(taps, axis=1), ws[3 * s], cfg["transposed"][3 * s])
        val = jnp.maximum(acc + params[5 * s + 1][...].reshape(1, -1), 0.0).astype(dtype)
        n = images * nc
        for ct in range(dst.shape[0]):
            l1 = min(chans[s + 1] - ct * LANE, LANE)
            r = 0
            for a, b in rows:
                part = val[r * n:(r + b - a) * n, ct * LANE:ct * LANE + l1]
                dst[ct, a + 1:b + 1, pl.ds(c0 + 1, nc), :, 0:l1] = part.reshape(b - a, nc, images, l1)
                r += b - a

    def conv(s, rows, c0, nc=1):
        src = ys[s]
        wait_load(3 * s + 1)
        wait_load(3 * s + 2)
        taps = []
        for kh in range(3):
            for kw in range(3):
                for ct in range(src.shape[0]):
                    taps.append(stack([flat(src[ct, a + kh:b + kh, pl.ds(c0 + kw, nc)]) for a, b in rows]))
        acc = times(jnp.concatenate(taps, axis=1), ws[3 * s + 1], cfg["transposed"][3 * s + 1])
        acc += times(centre(s, rows, c0, nc), ws[3 * s + 2], cfg["transposed"][3 * s + 2])
        val = jnp.maximum(acc + params[5 * s + 3][...].reshape(1, -1), 0.0).astype(dtype)
        n = images * nc
        if s == 2:
            (a, b), = rows
            out_ref[a:b] = val.reshape(b - a, images, chans[3])
            return
        dst = zin[s + 1]
        for ct in range(dst.shape[0]):
            l1 = min(chans[s + 1] - ct * LANE, LANE)
            r = 0
            for a, b in rows:
                part = val[r * n:(r + b - a) * n, ct * LANE:ct * LANE + l1].reshape(b - a, nc, images, l1)
                r += b - a
                even, odd = a + a % 2, b - b % 2
                for j in range(nc):
                    into = (lax.div(c0 + j, 2) + 1, lax.rem(c0 + j, 2), slice(None), slice(0, l1))
                    if a < even:
                        dst[(ct, a // 2 + 1, 1) + into] = part[0, j]
                    if odd > even:
                        dst[(ct, slice(even // 2 + 1, odd // 2 + 1), slice(None)) + into] = part[even - a:odd - a, j].reshape((odd - even) // 2, 2, images, l1)
                    if odd < b and b - 1 >= even:
                        dst[(ct, odd // 2 + 1, 0) + into] = part[b - 1 - a, j]

    def halves(tile):
        return pltpu.roll(tile.astype(jnp.float32), LANE // 2, tile.ndim - 1).astype(dtype)

    lower = lax.broadcasted_iota(jnp.int32, (1, images, LANE), 2) < LANE // 2

    def send_column(ex, key, side, packed, own, there, last, count):
        full = last + 1 if packed is None else last
        if packed is None:
            ex.send(key, 0, side, own(slice(0, full)), there(slice(0, full)))
        else:
            out, into = packed

            def pack():
                rest = own(full)[...].reshape(count // 2, 2, images, LANE)
                out[...] = jnp.where(lower, rest[:, 0], halves(rest[:, 1]))

            ex.send(key, 0, side, own(slice(0, full)), there(slice(0, full)), pack, ((key + ("rest",), out, into),))
        ex.landing[key] = (there(last), packed)

    def need_column(ex, key):
        if key in ex.waited:
            return
        into, packed = ex.landing[key]
        if packed is None:
            ex.need(key)
            return

        def unpack():
            tile = packed[1][...]
            none = jnp.zeros_like(tile)
            rest = jnp.stack([jnp.where(lower, tile, none), jnp.where(lower, halves(tile), none)], axis=1)
            into[...] = rest.reshape(into.shape)

        ex.need(key, key + ("rest",), after=unpack)

    def packs_of(key, a, b):
        if key not in PACKS:
            return None
        return tuple(packs.at[way, PACKS.index(key), a // 2:b // 2] for way in range(2))

    def send_y_col(s, name, side, k, own, there):
        a, b = ycuts[s][k]
        y = ys[s]
        packed = packs_of(("y", s, name), a, b)
        send_column(exchanges[2 * s + 1], (name, k), side, packed, lambda ct: y.at[ct, 1 + a:1 + b, 1 + own],
                    lambda ct: y.at[ct, 1 + a:1 + b, 1 + there], y.shape[0] - 1, b - a)

    def send_z_col(s, name, side, k, own, there):
        a, b = zcuts[s][k]
        z = zin[s]
        rows = slice(1 + a // 2, 1 + b // 2)
        packed = packs_of(("z", s, name), a, b)
        send_column(exchanges[2 * s], (name, k), side, packed, lambda ct: z.at[ct, rows, :, (own + 2) // 2, own % 2],
                    lambda ct: z.at[ct, rows, :, (there + 2) // 2, there % 2], z.shape[0] - 1, b - a)

    def send_y_rows(s, side):
        y, h, w = ys[s], height[s + 1], width[s + 1]
        own, there = (h, 0) if side > 0 else (1, h + 1)
        ex = exchanges[2 * s + 1]
        ex.send(("row", "r", side), side, 0, y.at[:, own, 1:w + 1], y.at[:, there, 1:w + 1])
        ex.send(("corner", "left", side), side, 1, y.at[:, own, w], y.at[:, there, 0])
        ex.send(("corner", "right", side), side, -1, y.at[:, own, 1], y.at[:, there, w + 1])

    def send_z_rows(s):
        z, h, w = zin[s], height[s] // 2, width[s] // 2
        ex = exchanges[2 * s]
        ex.send("row", 1, 0, z.at[:, h, 1, 1:], z.at[:, 0, 1, 1:])
        ex.send("corner", 1, 1, z.at[:, h, 1, w, 1], z.at[:, 0, 1, 0, 1])

    def need_corners(s, name):
        exchanges[2 * s + 1].need(("corner", name, -1), ("corner", name, 1))

    def need_z(s, name, b):
        for k, (lo, hi) in enumerate(zcuts[s]):
            if lo < 2 * b:
                need_column(exchanges[2 * s], (name, k))

    def need_y(s, name, b):
        for k, (lo, hi) in enumerate(ycuts[s]):
            if lo < b + 1:
                need_column(exchanges[2 * s + 1], (name, k))

    def blocks(lo, hi, size):
        return [[(k, min(k + size, hi))] for k in range(lo, hi, size)]

    zcuts = [cut(height[s], cfg["zcut"][s], 2) for s in range(3)]
    ycuts = [cut(height[s + 1], cfg["ycut"][s], 2) for s in range(3)]

    def turn(k):
        xloads[k].wait()
        for i in range(*zcuts[0][k]):
            tile = jnp.swapaxes(raw[:, i], 0, 1)
            xs[0, i // 2 + 1, i % 2, 1:1 + width[0] // 2] = tile.reshape(width[0] // 2, 2, images, LANE)

    turn(0)
    row_inner = jnp.logical_and(row > 0, row + 1 < cfg["rows"])
    col_inner = jnp.logical_and(col > 0, col + 1 < cfg["cols"])
    for rows, row_test in ((3, row_inner), (2, jnp.logical_not(row_inner))):
        for cols, col_test in ((3, col_inner), (2, jnp.logical_not(col_inner))):
            pl.when(jnp.logical_and(row_test, col_test))(functools.partial(pl.semaphore_wait, barrier, rows * cols - 1))

    w0, w1, w2 = width[:3]
    h1, h2, h3 = height[1:]
    for k in range(len(zcuts[0])):
        if k:
            turn(k)
        send_z_col(0, "left", 1, k, w0 - 1, -1)
    send_z_rows(0)

    ex = exchanges[0]
    for rows in blocks(8, h1, 8):
        down(0, rows, 1, w1 - 1)
    ex.need("row")
    down(0, [(0, 8)], 1, w1 - 1)
    for k in range(len(ycuts[0])):
        send_y_col(0, "left", 1, k, w1 - 1, -1)
    for k, (a, b) in enumerate(ycuts[0]):
        need_z(0, "left", b)
        ex.need("corner")
        down(0, [(a, b)], 0)
        send_y_col(0, "right", -1, k, 0, w1)
        if k == 0:
            send_y_rows(0, -1)
        if b == h1:
            send_y_rows(0, 1)
        for rows in blocks(max(a - 1, 1), b - 1, 8):
            conv(0, rows, 1, w1 - 2)
    exchanges[1].need(("row", "r", -1), ("row", "r", 1))
    conv(0, [(0, 1), (h1 - 1, h1)], 1, w1 - 2)
    need_corners(0, "right")
    for k, (a, b) in enumerate(zcuts[1]):
        need_y(0, "right", b)
        conv(0, [(a, b)], w1 - 1)
        send_z_col(1, "left", 1, k, w1 - 1, -1)
    need_corners(0, "left")
    for k, (a, b) in enumerate(zcuts[1]):
        need_y(0, "left", b)
        conv(0, [(a, b)], 0)
    send_z_rows(1)

    ex = exchanges[2]
    ex.need("row")
    for rows in blocks(0, h2, 12):
        down(1, rows, 1, w2 - 1)
    for k, (a, b) in enumerate(ycuts[1]):
        need_z(1, "left", b)
        ex.need("corner")
        down(1, [(a, b)], 0)
        send_y_col(1, "right", -1, k, 0, w2)
        send_y_col(1, "left", 1, k, w2 - 1, -1)
        if k == 0:
            send_y_rows(1, -1)
        if b == h2:
            send_y_rows(1, 1)
    exchanges[3].need(("row", "r", -1), ("row", "r", 1))
    need_corners(1, "right")
    for k, (a, b) in enumerate(zcuts[2]):
        need_y(1, "right", b)
        conv(1, [(a, b)], 1, w2 - 1)
        send_z_col(2, "left", 1, k, w2 - 1, -1)
    need_corners(1, "left")
    for k, (a, b) in enumerate(zcuts[2]):
        need_y(1, "left", b)
        conv(1, [(a, b)], 0)
    send_z_rows(2)

    ex = exchanges[4]
    ex.need("row")
    for k, (a, b) in enumerate(ycuts[2]):
        need_z(2, "left", b)
        ex.need("corner")
        down(2, [(a, b)], 0)
        send_y_col(2, "right", -1, k, 0, 1)
        send_y_col(2, "left", 1, k, 0, -1)
        if k == 0:
            send_y_rows(2, -1)
        if b == h3:
            send_y_rows(2, 1)
    exchanges[5].need(("row", "r", -1), ("row", "r", 1))
    need_corners(2, "left")
    need_corners(2, "right")
    need_y(2, "left", h3)
    need_y(2, "right", h3)
    conv(2, [(0, h3)], 0)
    assert counter[0] == sems.shape[1]
    groups = {}
    for ex in exchanges:
        for test, wait in ex.sends():
            groups.setdefault(id(test), (test, []))[1].append(wait)
    ex.together(groups.values())


def solution(mesh):
    row_count = mesh.shape["row"]
    col_count = mesh.shape["col"]
    tile_spec = P("batch", "row", "col")

    def local_blocks(x_tile, *params):
        images, tile_h, tile_w, c0 = x_tile.shape
        chans = [c0] + [params[5 * s].shape[-1] for s in range(3)]
        height = [tile_h >> s for s in range(4)]
        width = [tile_w >> s for s in range(4)]
        operands, transposed, wshapes = [], [], []
        for s in range(3):
            for p in range(5):
                value = params[5 * s + p]
                if p in (1, 3):
                    operands.append(value)
                    continue
                k, n = value.shape[-2:]
                flip = k % LANE == 0 and n % LANE != 0
                value = value.reshape(-1, k, n)
                if flip:
                    value = jnp.swapaxes(value, 1, 2)
                    wshapes.append(value.shape)
                else:
                    wshapes.append((value.shape[0], tiles_of(k) * LANE, n))
                operands.append(value)
                transposed.append(flip)
        zcut, ycut = (4, 3, 3), (4, 3, 2)
        cfg = dict(chans=chans, height=height, width=width, rows=row_count, cols=col_count, images=images, transposed=transposed, zcut=zcut, ycut=ycut)
        messages = 65
        bf16 = jnp.bfloat16
        scratch = [pltpu.VMEM(x_tile.shape, bf16), pltpu.VMEM((1, tile_h // 2 + 1, 2, tile_w // 2 + 1, 2, images, LANE), bf16)]
        for s in (1, 2, 3):
            scratch.append(pltpu.VMEM((tiles_of(chans[s]), height[s] + 2, width[s] + 2, images, LANE), bf16))
        for s in (1, 2):
            scratch.append(pltpu.VMEM((tiles_of(chans[s]), height[s] // 2 + 1, 2, width[s] // 2 + 1, 2, images, LANE), bf16))
        for shape in wshapes:
            scratch.append(pltpu.VMEM(shape, bf16))
        scratch.append(pltpu.VMEM((2, len(PACKS), height[2] // 2, images, LANE), bf16))
        scratch += [pltpu.SemaphoreType.DMA((9 + zcut[0],)), pltpu.SemaphoreType.DMA((2, messages))]
        hbm = pl.BlockSpec(memory_space=pl.ANY)
        vmem = pl.BlockSpec(memory_space=pltpu.VMEM)
        out = pl.pallas_call(
            functools.partial(body, cfg),
            out_shape=jax.ShapeDtypeStruct((height[3], images, chans[3]), bf16),
            in_specs=[hbm] + [vmem if p in (1, 3) else hbm for _ in range(3) for p in range(5)],
            out_specs=vmem,
            scratch_shapes=scratch,
            compiler_params=pltpu.CompilerParams(collective_id=0, has_side_effects=True, vmem_limit_bytes=60 * 1024 * 1024),
            name="encoder",
        )(x_tile, *operands)
        return jnp.transpose(out, (1, 0, 2))[:, :, None, :]

    return jax.shard_map(local_blocks, mesh=mesh, in_specs=(tile_spec,) + (P(),) * 15, out_specs=tile_spec, check_vma=False)
```

```python
import functools

import jax
import jax.numpy as jnp
from jax import lax
from jax.experimental import pallas as pl
from jax.experimental.pallas import tpu as pltpu
from jax.sharding import PartitionSpec as P

LANE = 128
MESH = pl.DeviceIdType.MESH
NEIGHBOURS = [(dr, dc) for dr in range(-1, 2) for dc in range(-1, 2) if dr or dc]


def tiles_of(channels):
    return -(-channels // LANE)


def pair(index):
    return index // 2 + 1, index % 2


def cut(count, pieces):
    bounds = [0] + [(count * k // pieces + 2) // 2 * 2 for k in range(1, pieces)] + [count]
    return list(zip(bounds, bounds[1:]))


WEIGHTS = (0, 2, 4)
TAPS = range(3)
LEFT, MIDDLE, RIGHT = (0,), (1,), (2,)
INNER, LOCAL = LEFT + MIDDLE, MIDDLE + RIGHT
PACKS = [("y", s, name) for s in range(1, 3) for name in ("left", "right")] + [("z", 2, "left")]


class Exchange:
    def __init__(self, grid, sems, counter, known):
        self.grid, self.sems, self.counter = grid, sems, counter
        self.copies = {}
        self.known = known
        self.landing = {}
        self.waited = set()

    def exists(self, dr, dc):
        if (dr, dc) not in self.known:
            row, col, row_count, col_count = self.grid
            tests = []
            if dr:
                tests.append(row + 1 < row_count if dr > 0 else row > 0)
            if dc:
                tests.append(col + 1 < col_count if dc > 0 else col > 0)
            self.known[dr, dc] = functools.reduce(jnp.logical_and, tests)
        return self.known[dr, dc]

    def arrives(self, key):
        dr, dc = self.copies[key][1:]
        return self.exists(-dr, -dc)

    def send(self, key, dr, dc, src, dst, before=None, then=None):
        row, col = self.grid[:2]
        copies = []
        for name, source, target in ((key, src, dst),) + (then or ()):
            index = self.counter[0]
            self.counter[0] += 1
            copy = pltpu.make_async_remote_copy(
                src_ref=source, dst_ref=target, send_sem=self.sems.at[0, index], recv_sem=self.sems.at[1, index],
                device_id={"row": row + dr, "col": col + dc}, device_id_type=MESH)
            self.copies[name] = (copy, dr, dc)
            copies.append(copy)

        def start():
            copies[0].start()
            if before is not None:
                before()
            for copy in copies[1:]:
                copy.start()

        pl.when(self.exists(dr, dc))(start)

    def together(self, groups):
        for test, waits in groups:
            def wait(waits=waits):
                for one in waits:
                    one()

            pl.when(test)(wait)

    def need(self, *keys, after=None):
        groups = {}
        for key in keys:
            if key not in self.waited:
                self.waited.add(key)
                test = self.arrives(key)
                groups.setdefault(id(test), (test, []))[1].append(self.copies[key][0].wait_recv)
        if after is not None:
            for test, waits in groups.values():
                waits.append(after)
        self.together(groups.values())

    def sends(self):
        assert self.waited == set(self.copies)
        return [(self.exists(dr, dc), copy.wait_send) for copy, dr, dc in self.copies.values()]


def body(cfg, x_hbm, *refs):
    params, refs = refs[:15], refs[15:]
    out_ref, raw, xs, y1, y2, y3, z1, z2, *ws, packs, accs, load_sems, sems = refs
    ys, zs = (y1, y2, y3), (z1, z2)
    w_down, w_conv, w_proj = (list(zip(ws, cfg["transposed"]))[k::3] for k in range(3))
    b_down, b_conv = (params[k::5] for k in (1, 3))
    chans, height, width = cfg["chans"], cfg["height"], cfg["width"]
    row, col = lax.axis_index("row"), lax.axis_index("col")
    grid = (row, col, cfg["rows"], cfg["cols"])
    counter = [0]
    known = {}
    dtype = jnp.bfloat16
    images = cfg["images"]

    xcuts = cut(height[1], cfg["pieces"][0])
    xloads = [pltpu.make_async_copy(x_hbm.at[:, 2 * a:2 * b], raw.at[:, 2 * a:2 * b], load_sems.at[9 + k]) for k, (a, b) in enumerate(xcuts)]
    loads = []
    for stage in range(3):
        for k, p in enumerate(WEIGHTS):
            src, dst = params[5 * stage + p], ws[3 * stage + k]
            if dst.shape != src.shape:
                dst = dst.at[:, :src.shape[1]]
            loads.append(pltpu.make_async_copy(src, dst, load_sems.at[3 * stage + k]))
    for load in xloads + loads[:3]:
        load.start()

    def zero(ref):
        ref[...] = jnp.zeros(ref.shape, ref.dtype)

    for buf in (xs,) + tuple(zs):
        zero(buf.at[:, 0, 1])
        zero(buf.at[:, :, :, 0, 1])
    for s, buf in enumerate(ys):
        zero(buf.at[:, 0:1])
        zero(buf.at[:, -1:])
        zero(buf.at[:, :, 0:1])
        zero(buf.at[:, :, width[s + 1] + 1:])
    for buf in tuple(ys[1:]) + tuple(zs[1:]):
        zero(buf.at[buf.shape[0] - 1:])
    for k, p in enumerate(WEIGHTS * 3):
        src, dst = params[5 * (k // 3) + p], ws[k]
        if dst.shape != src.shape:
            zero(dst.at[:, src.shape[1]:])

    for load in loads[3:]:
        load.start()

    exchanges = [Exchange(grid, sems, counter, known) for _ in range(6)]
    barrier = pltpu.get_barrier_semaphore()
    for dr, dc in NEIGHBOURS:
        there = exchanges[0].exists(dr, dc)

        def greet(dr=dr, dc=dc):
            pl.semaphore_signal(barrier, inc=1, device_id={"row": row + dr, "col": col + dc}, device_id_type=MESH)

        pl.when(there)(greet)
    zin = [xs, zs[0], zs[1]]

    waited_loads = set()

    def wait_load(index):
        if index not in waited_loads:
            waited_loads.add(index)
            loads[index].wait()

    def flat(block):
        return block.reshape(-1, LANE)

    def stack(pieces):
        return pieces[0] if len(pieces) == 1 else jnp.concatenate(pieces, axis=0)

    def times(taps, ref, transposed):
        if transposed:
            return sum(lax.dot_general(lhs, ref[t], (((1,), (1,)), ((), ())), preferred_element_type=jnp.float32) for t, lhs in taps)
        lhs = jnp.concatenate([lhs for _, lhs in taps], axis=1)
        return jnp.dot(lhs, stack([ref[t] for t, _ in taps]), preferred_element_type=jnp.float32)

    def partial_sum(slot, rows, acc, keep):
        r = 0
        parts = []
        for a, b in rows:
            n = (b - a) * images
            if keep == "first":
                accs[slot, a * images:b * images] = acc[r:r + n]
            else:
                parts.append(accs[slot, a * images:b * images])
            r += n
        return None if keep == "first" else acc + stack(parts)

    def strided(src, ct, runs, kh, kw, c0, nc):
        up, lo = (1 if kh else 0), c0 + (1 if kw else 0)
        return stack([flat(src[ct, a + up:b + up, (kh + 1) % 2, pl.ds(lo, nc), (kw + 1) % 2]) for a, b in runs])

    def centre(s, runs, c0, nc):
        src = zin[s]
        return jnp.concatenate([strided(src, ct, runs, 1, 1, c0, nc) for ct in range(src.shape[0])], axis=1)

    def down(s, rows, c0, nc=1, kws=TAPS, keep=None):
        src, dst = zin[s], ys[s]
        wait_load(3 * s)
        taps = []
        for kh in TAPS:
            for kw in kws:
                taps.append((3 * kh + kw, jnp.concatenate([strided(src, ct, rows, kh, kw, c0, nc) for ct in range(src.shape[0])], axis=1)))
        acc = times(taps, *w_down[s])
        if keep:
            acc = partial_sum(2 * s - 2, rows, acc, keep)
            if acc is None:
                return
        val = jnp.maximum(acc + b_down[s][...].reshape(1, -1), 0.0).astype(dtype)
        n = images * nc
        for ct in range(dst.shape[0]):
            l1 = min(chans[s + 1] - ct * LANE, LANE)
            r = 0
            for a, b in rows:
                part = val[r * n:(r + b - a) * n, ct * LANE:ct * LANE + l1]
                dst[ct, a + 1:b + 1, pl.ds(c0 + 1, nc), :, 0:l1] = part.reshape(b - a, nc, images, l1)
                r += b - a

    def conv(s, rows, c0, nc=1, kws=TAPS, keep=None):
        src = ys[s]
        wait_load(3 * s + 1)
        wait_load(3 * s + 2)
        taps = []
        for kh in TAPS:
            for kw in kws:
                taps.append((3 * kh + kw, jnp.concatenate([stack([flat(src[ct, a + kh:b + kh, pl.ds(c0 + kw, nc)]) for a, b in rows]) for ct in range(src.shape[0])], axis=1)))
        acc = times(taps, *w_conv[s])
        if keep != "rest":
            acc += times([(0, centre(s, rows, c0, nc))], *w_proj[s])
        if keep:
            acc = partial_sum(2 * s - 1, rows, acc, keep)
            if acc is None:
                return
        val = jnp.maximum(acc + b_conv[s][...].reshape(1, -1), 0.0).astype(dtype)
        n = images * nc
        if s == 2:
            (a, b), = rows
            out_ref[a:b] = val.reshape(b - a, images, chans[3])
            return
        dst = zin[s + 1]
        for ct in range(dst.shape[0]):
            l1 = min(chans[s + 1] - ct * LANE, LANE)
            r = 0
            for a, b in rows:
                part = val[r * n:(r + b - a) * n, ct * LANE:ct * LANE + l1].reshape(b - a, nc, images, l1)
                r += b - a
                even, odd = a + a % 2, b - b % 2
                for j in range(nc):
                    into = pair(c0 + j) + (slice(None), slice(l1))
                    if a < even:
                        dst[(ct,) + pair(a) + into] = part[0, j]
                    if odd > even:
                        dst[(ct, slice(even // 2 + 1, odd // 2 + 1), slice(None)) + into] = part[even - a:odd - a, j].reshape((odd - even) // 2, 2, images, l1)
                    if odd < b and b - 1 >= even:
                        dst[(ct,) + pair(odd) + into] = part[odd - a, j]

    def halves(tile):
        return pltpu.roll(tile.astype(jnp.float32), LANE // 2, tile.ndim - 1).astype(dtype)

    lower = lax.broadcasted_iota(jnp.int32, (1, images, LANE), 2) < LANE // 2

    def send_column(ex, key, side, packed, own, there, last, count):
        full = last + 1 if packed is None else last
        if packed is None:
            ex.send(key, 0, side, own(slice(0, full)), there(slice(0, full)))
        else:
            out, into = packed

            def pack():
                rest = own(full)[...].reshape(count // 2, 2, images, LANE)
                out[...] = jnp.where(lower, rest[:, 0], halves(rest[:, 1]))

            ex.send(key, 0, side, own(slice(0, full)), there(slice(0, full)), pack, ((key + ("rest",), out, into),))
        ex.landing[key] = (there(last), packed)

    def need_column(ex, key):
        if key in ex.waited:
            return
        into, packed = ex.landing[key]
        if packed is None:
            ex.need(key)
            return

        def unpack():
            tile = packed[1][...]
            none = jnp.zeros_like(tile)
            rest = jnp.stack([jnp.where(lower, tile, none), jnp.where(lower, halves(tile), none)], axis=1)
            into[...] = rest.reshape(into.shape)

        ex.need(key, key + ("rest",), after=unpack)

    def packs_of(key, a, b):
        if key not in PACKS:
            return None
        return tuple(packs.at[way, PACKS.index(key), a // 2:b // 2] for way in range(2))

    def send_y_col(s, name, side, k, own, there):
        a, b = ycuts[s][k]
        y = ys[s]
        rows = slice(1 + a, 1 + b)
        packed = packs_of(("y", s, name), a, b)
        send_column(exchanges[2 * s + 1], (name, k), side, packed, lambda ct: y.at[ct, rows, 1 + own],
                    lambda ct: y.at[ct, rows, 1 + there], y.shape[0] - 1, b - a)

    def send_z_col(s, name, side, k, own, there):
        a, b = zcuts[s][k]
        z = zin[s]
        rows = slice(1 + a // 2, 1 + b // 2)
        packed = packs_of(("z", s, name), a, b)
        send_column(exchanges[2 * s], (name, k), side, packed, lambda ct: z.at[(ct, rows, slice(None)) + pair(own)],
                    lambda ct: z.at[(ct, rows, slice(None)) + pair(there)], z.shape[0] - 1, b - a)

    def send_y_rows(s, side):
        y, h, w = ys[s], height[s + 1], width[s + 1]
        own, there = (h, 0) if side > 0 else (1, h + 1)
        ex = exchanges[2 * s + 1]
        ex.send(("row", "r", side), side, 0, y.at[:, own, 1:w + 1], y.at[:, there, 1:w + 1])
        ex.send(("corner", "left", side), side, 1, y.at[:, own, w], y.at[:, there, 0])
        ex.send(("corner", "right", side), side, -1, y.at[:, own, 1], y.at[:, there, w + 1])

    def send_z_rows(s):
        z, h, w = zin[s], height[s] // 2, width[s] // 2
        ex = exchanges[2 * s]
        ex.send("row", 1, 0, z.at[:, h, 1, 1:], z.at[:, 0, 1, 1:])
        ex.send("corner", 1, 1, z.at[:, h, 1, w, 1], z.at[:, 0, 1, 0, 1])

    def need_corners(s, name):
        exchanges[2 * s + 1].need(("corner", name, -1), ("corner", name, 1))

    def need_z(s, name, b):
        for k, (lo, hi) in enumerate(zcuts[s]):
            if lo < 2 * b:
                need_column(exchanges[2 * s], (name, k))

    def need_y(s, name, b):
        for k, (lo, hi) in enumerate(ycuts[s]):
            if lo < b + 1:
                need_column(exchanges[2 * s + 1], (name, k))

    def blocks(lo, hi, size):
        return [[(k, min(k + size, hi))] for k in range(lo, hi, size)]

    ycuts = [cut(height[s + 1], pieces) for s, pieces in enumerate(cfg["pieces"])]
    zcuts = [[(2 * a, 2 * b) for a, b in cuts] for cuts in ycuts]

    def turn(k):
        xloads[k].wait()
        for i in range(*zcuts[0][k]):
            tile = jnp.swapaxes(raw[:, i], 0, 1)
            xs[(0,) + pair(i) + (slice(1, None),)] = tile.reshape(width[0] // 2, 2, images, LANE)

    turn(0)
    row_inner = jnp.logical_and(row > 0, row + 1 < cfg["rows"])
    col_inner = jnp.logical_and(col > 0, col + 1 < cfg["cols"])
    for rows, row_test in ((3, row_inner), (2, jnp.logical_not(row_inner))):
        for cols, col_test in ((3, col_inner), (2, jnp.logical_not(col_inner))):
            pl.when(jnp.logical_and(row_test, col_test))(functools.partial(pl.semaphore_wait, barrier, rows * cols - 1))

    w0, w1, w2 = width[:3]
    h1, h2, h3 = height[1:]
    for k in range(len(zcuts[0])):
        if k:
            turn(k)
        send_z_col(0, "left", 1, k, w0 - 1, -1)
    send_z_rows(0)

    ex = exchanges[0]
    for rows in blocks(8, h1, 8):
        down(0, rows, 1, w1 - 1)
    ex.need("row")
    down(0, [(0, 8)], 1, w1 - 1)
    for k in range(len(ycuts[0])):
        send_y_col(0, "left", 1, k, w1 - 1, -1)
    for k, (a, b) in enumerate(ycuts[0]):
        need_z(0, "left", b)
        ex.need("corner")
        down(0, [(a, b)], 0)
        send_y_col(0, "right", -1, k, 0, w1)
        if k == 0:
            send_y_rows(0, -1)
        if b == h1:
            send_y_rows(0, 1)
        for rows in blocks(max(a - 1, 1), b - 1, 8):
            conv(0, rows, 1, w1 - 2)
    exchanges[1].need(("row", "r", -1), ("row", "r", 1))
    conv(0, [(0, 1), (h1 - 1, h1)], 1, w1 - 2)
    need_corners(0, "right")
    for k, (a, b) in enumerate(zcuts[1]):
        need_y(0, "right", b)
        conv(0, [(a, b)], w1 - 1)
        send_z_col(1, "left", 1, k, w1 - 1, -1)
    need_corners(0, "left")
    for k, (a, b) in enumerate(zcuts[1]):
        need_y(0, "left", b)
        conv(0, [(a, b)], 0)
    send_z_rows(1)

    ex = exchanges[2]
    ex.need("row")
    for rows in blocks(0, h2, 12):
        down(1, rows, 1, w2 - 1)
    down(1, [(0, h2)], 0, kws=LOCAL, keep="first")
    for k, (a, b) in enumerate(ycuts[1]):
        need_z(1, "left", b)
        ex.need("corner")
        down(1, [(a, b)], 0, kws=LEFT, keep="rest")
        send_y_col(1, "right", -1, k, 0, w2)
        send_y_col(1, "left", 1, k, w2 - 1, -1)
        if k == 0:
            send_y_rows(1, -1)
        if b == h2:
            send_y_rows(1, 1)
    conv(1, [(1, h2 - 1)], 1, kws=INNER, keep="first")
    exchanges[3].need(("row", "r", -1), ("row", "r", 1))
    conv(1, [(0, 1), (h2 - 1, h2)], 1, kws=INNER, keep="first")
    need_corners(1, "right")
    for k, (a, b) in enumerate(zcuts[2]):
        need_y(1, "right", b)
        conv(1, [(a, b)], 1, kws=RIGHT, keep="rest")
        send_z_col(2, "left", 1, k, w2 - 1, -1)
    need_corners(1, "left")
    for k, (a, b) in enumerate(zcuts[2]):
        need_y(1, "left", b)
        conv(1, [(a, b)], 0)
    send_z_rows(2)

    ex = exchanges[4]
    ex.need("row")
    down(2, [(0, h3)], 0, kws=LOCAL, keep="first")
    for k, (a, b) in enumerate(ycuts[2]):
        need_z(2, "left", b)
        ex.need("corner")
        down(2, [(a, b)], 0, kws=LEFT, keep="rest")
        send_y_col(2, "right", -1, k, 0, 1)
        send_y_col(2, "left", 1, k, 0, -1)
        if k == 0:
            send_y_rows(2, -1)
        if b == h3:
            send_y_rows(2, 1)
    exchanges[5].need(("row", "r", -1), ("row", "r", 1))
    conv(2, [(0, h3)], 0, kws=MIDDLE, keep="first")
    need_corners(2, "left")
    need_corners(2, "right")
    need_y(2, "left", h3)
    need_y(2, "right", h3)
    conv(2, [(0, h3)], 0, kws=LEFT + RIGHT, keep="rest")
    assert counter[0] == sems.shape[1]
    groups = {}
    for ex in exchanges:
        for test, wait in ex.sends():
            groups.setdefault(id(test), (test, []))[1].append(wait)
    ex.together(groups.values())


def solution(mesh):
    row_count = mesh.shape["row"]
    col_count = mesh.shape["col"]
    tile_spec = P("batch", "row", "col")

    def local_blocks(x_tile, *params):
        images, tile_h, tile_w, c0 = x_tile.shape
        chans = [c0] + [params[5 * s].shape[-1] for s in range(3)]
        height = [tile_h >> s for s in range(4)]
        width = [tile_w >> s for s in range(4)]
        operands, transposed, wshapes = [], [], []
        for s in range(3):
            for p in range(5):
                value = params[5 * s + p]
                if p in (1, 3):
                    operands.append(value)
                    continue
                k, n = value.shape[-2:]
                flip = k % LANE == 0 and n % LANE != 0
                value = value.reshape(-1, k, n)
                if flip:
                    value = jnp.swapaxes(value, 1, 2)
                    wshapes.append(value.shape)
                else:
                    wshapes.append((value.shape[0], tiles_of(k) * LANE, n))
                operands.append(value)
                transposed.append(flip)
        pieces = (4, 4, 2)
        cfg = dict(chans=chans, height=height, width=width, rows=row_count, cols=col_count, images=images, transposed=transposed, pieces=pieces)
        messages = 24 + 3 * pieces[0] + 5 * pieces[1] + 6 * pieces[2]
        bf16 = jnp.bfloat16
        scratch = [pltpu.VMEM(x_tile.shape, bf16), pltpu.VMEM((1, tile_h // 2 + 1, 2, tile_w // 2 + 1, 2, images, LANE), bf16)]
        for s in (1, 2, 3):
            scratch.append(pltpu.VMEM((tiles_of(chans[s]), height[s] + 2, width[s] + 2, images, LANE), bf16))
        for s in (1, 2):
            scratch.append(pltpu.VMEM((tiles_of(chans[s]), height[s] // 2 + 1, 2, width[s] // 2 + 1, 2, images, LANE), bf16))
        for shape in wshapes:
            scratch.append(pltpu.VMEM(shape, bf16))
        scratch.append(pltpu.VMEM((2, len(PACKS), height[2] // 2, images, LANE), bf16))
        scratch.append(pltpu.VMEM((4, height[2] * images, chans[3]), jnp.float32))
        scratch += [pltpu.SemaphoreType.DMA((9 + pieces[0],)), pltpu.SemaphoreType.DMA((2, messages))]
        hbm = pl.BlockSpec(memory_space=pl.ANY)
        vmem = pl.BlockSpec(memory_space=pltpu.VMEM)
        out = pl.pallas_call(
            functools.partial(body, cfg),
            out_shape=jax.ShapeDtypeStruct((height[3], images, chans[3]), bf16),
            in_specs=[hbm] + [vmem if p in (1, 3) else hbm for _ in range(3) for p in range(5)],
            out_specs=vmem,
            scratch_shapes=scratch,
            compiler_params=pltpu.CompilerParams(collective_id=0, has_side_effects=True, vmem_limit_bytes=60 << 20),
            name="encoder",
        )(x_tile, *operands)
        return jnp.transpose(out, (1, 0, 2))[:, :, None, :]

    return jax.shard_map(local_blocks, mesh=mesh, in_specs=(tile_spec,) + (P(),) * 15, out_specs=tile_spec, check_vma=False)
```
